32 devices in a mesh: grp: 2 (over y), bank: 4 (over z), seg: 4 (over x, core).
Axes of the slice: x: 2, y: 2, z: 4, core: 2. Of those that a mesh axis runs over, the one named last changes fastest.
Arguments:
- strain: bfloat16 [32, 2, 32768], P(('grp', 'seg'), None, 'bank'), parts along dimension 0, may hold values from -6 to 6
- templates: bfloat16 [4, 2, 32768], P('bank'), may hold values from -6 to 6
- length_bins: int32 [4], P('bank'), may hold values from 0 to 3
Outputs:
- snr_table: float32 [4, 32], P('bank', ('grp', 'seg')), parts along dimension 1
- segment_peak: float32 [32], P(('grp', 'seg')), parts along dimension 0
- template_peak: float32 [8], P(('grp', 'bank')), parts along dimension 0
The draws below stay inside these ranges and needn't reach their ends.
There are 2 independent parts, one for each index of `grp`. The reference program is written for one: setup_inputs(seed, part) draws one part's arguments, and reference() takes and returns one part's arrays. A program takes and returns all parts, laid end to end along the dimension named above; an argument that names none is the same for every part. Nothing has to cross between parts.
All inputs are finite; a program needn't handle non-finite values.
Results may differ from the reference program's by a relative error of at most 0.0003.
Values may be sent and summed in bfloat16 or wider, within the bound.
A program may use at most 64 MiB of HBM per device.

```python
import jax
import jax.numpy as jnp
from jax import lax

LEN = 32768
TEMPLATES = 4
SEGMENTS = 16


def with_ends(result, stream_key, least, largest):
    longest = result.shape.index(max(result.shape))
    spots = []
    for shift in (0, 1):
        where = [jax.random.randint(jax.random.fold_in(stream_key, axis), (), 0, length) for axis, length in enumerate(result.shape)]
        where[longest] = (where[longest] + shift) % result.shape[longest]
        spots.append(tuple(where))
    return result.at[spots[0]].set(least).at[spots[1]].set(largest)


def block_scale(rng, shape, pieces, low, largest):
    level, own = 1.0, jax.random.fold_in(rng, 6)
    for axis_at, blocks in pieces:
        draws = jnp.exp(jax.random.uniform(jax.random.fold_in(own, axis_at), (blocks,), jnp.float32, low / len(pieces), largest / len(pieces)))
        level = level * jnp.repeat(draws, shape[axis_at] // blocks).reshape([-1 if axis == axis_at else 1 for axis in range(len(shape))])
    return level


def noise(stream_key, extent, scale, most, split=(), kind=jnp.bfloat16):
    entries = jax.random.normal(stream_key, extent, jnp.float32) * scale
    if len(split) > 0:
        entries = block_scale(stream_key, extent, split, -0.22, 0.18) * entries
    return jnp.clip(entries, min=-most, max=most).astype(kind)


def setup_inputs(seed: int = 0, part: int = 0) -> dict:
    splits = jax.random.split(jax.random.key(seed), 4)
    part_keys = jax.random.split(jax.random.fold_in(splits[3], part), 4)
    strain = noise(part_keys[0], (SEGMENTS, 2, LEN), 1.0, 6.0, ((0, 4), (2, 4)))
    templates = noise(splits[1], (TEMPLATES, 2, LEN), 1.0, 6.0, ((0, 4),))
    length_bins = with_ends(jax.random.randint(splits[2], (TEMPLATES,), 0, 4), jax.random.fold_in(splits[2], 1), 0, 3).astype(jnp.int32)
    return {"strain": strain, "templates": templates, "length_bins": length_bins}


EPSILON = 1e-06

def reference(strain, templates, length_bins):
    seg_real = strain[:, 0, :].astype(jnp.float32)
    seg_imag = strain[:, 1, :].astype(jnp.float32)
    positions = jnp.arange(LEN, dtype=jnp.int32)

    def one_template(inputs):
        template, length_bin = inputs
        cutoff = jnp.right_shift(jnp.int32(LEN), length_bin.astype(jnp.int32))
        keep_mask = positions < cutoff
        tpl_real = jnp.where(keep_mask, template[0].astype(jnp.float32), 0.0)
        tpl_imag = jnp.where(keep_mask, template[1].astype(jnp.float32), 0.0)
        norm_value = jnp.sqrt(jnp.sum(tpl_real * tpl_real + tpl_imag * tpl_imag) + EPSILON)
        prod_real = tpl_real * seg_real + tpl_imag * seg_imag
        prod_imag = tpl_real * seg_imag - tpl_imag * seg_real
        series = jnp.fft.ifft(prod_real + 1j * prod_imag, axis=-1) * LEN
        peak_power = lax.optimization_barrier(jnp.max(jnp.real(series) ** 2 + jnp.imag(series) ** 2, axis=-1))
        return jnp.sqrt(peak_power) / norm_value
    snr_table = lax.map(one_template, (templates, length_bins))
    return (snr_table, lax.optimization_barrier(jnp.max(snr_table, axis=0)), lax.optimization_barrier(jnp.max(snr_table, axis=1)))
```

```python
import functools
import math

import jax
import jax.numpy as jnp
import numpy as np
from jax import lax
from jax.experimental import pallas as pl
from jax.experimental.pallas import tpu as pltpu
from jax.sharding import PartitionSpec as P

MESH = pl.DeviceIdType.MESH
EPSILON = 1e-06
LANES = 128
GRANT = 56492032


def split(value):
    high = value.astype(jnp.bfloat16)
    low = (value - high.astype(jnp.float32)).astype(jnp.bfloat16)
    return high, low


def tables(length):
    rows = length // LANES
    half = rows // 2

    def root(phase, period):
        angle = 2.0 * math.pi * (phase % period) / period
        return np.cos(angle), np.sin(angle)

    r = np.arange(half)
    c = np.arange(LANES)
    row_c, row_s = root(np.outer(r, r), half)
    first = np.block([[row_c, -row_s], [row_s, row_c]])
    col_c, col_s = root(np.outer(c, c), LANES)
    last = np.block([[col_c, col_s], [-col_s, col_c]])
    odd = np.stack([np.broadcast_to(part[:, None], (half, LANES)) for part in root(r, rows)])
    turn = [root(np.outer(2 * r + p, c), length) for p in (0, 1)]
    turn = np.stack([np.concatenate([turn[0][i], turn[1][i]], axis=1) for i in (0, 1)])

    def halves(matrix):
        high = matrix.astype(jnp.bfloat16)
        low = (matrix - high.astype(np.float64)).astype(jnp.bfloat16)
        return high, low

    f_high, f_low = halves(first)
    l_high, l_low = halves(last)
    first = np.concatenate([f_high, f_high, f_low], axis=1)
    last = np.concatenate([l_high, l_high, l_low], axis=0)
    return first, last, odd.astype(np.float32), turn.astype(np.float32)


def kernel(
    banks, segs, chunks, give,
    strain_hbm, tpl_hbm, bins_ref, first_hbm, last_hbm, odd_hbm, turn_hbm,
    out_ref,
    strain_ref, tpl_ref, masked, lent, held, tpl_re, tpl_im, two_re, two_im, work, first, last, odd, turn,
    row_bank, row_seg, row_far,
    input_sem, table_sem, right_sem, left_sem, recv_sem, bank_send, bank_recv, seg_send, seg_recv,
    far_send, far_recv, tpl_send, tpl_recv,
):
    me = lax.axis_index("bank")
    my_seg = lax.axis_index("seg")
    count, depth, _ = strain_ref.shape
    size = count // chunks
    rows = tpl_ref.shape[0] // 2
    half = rows // 2

    def part(chunk):
        return pl.ds(chunk * size, size)

    barrier = pltpu.get_barrier_semaphore()
    has_left, has_right = me > 0, me < banks - 1
    is_end = jnp.logical_not(has_left & has_right) & (give > 0)
    helps = ((me == 1) | (me == banks - 2)) & (give > 0)
    helper = jnp.where(me == 0, 1, banks - 2)
    helped = jnp.where(me == 1, 0, banks - 1)

    def wanted(device, chunk):
        least = 1 if chunk >= chunks - give else 0
        return (device >= least) & (device < banks - least)


    @pl.when(has_left)
    def _():
        pl.semaphore_signal(barrier, inc=1, device_id={"bank": me - 1}, device_id_type=MESH)

    @pl.when(has_right)
    def _():
        pl.semaphore_signal(barrier, inc=1, device_id={"bank": me + 1}, device_id_type=MESH)

    for step in range(1, segs):
        pl.semaphore_signal(
            barrier, inc=1, device_id={"seg": lax.rem(my_seg + step, segs)}, device_id_type=MESH
        )
    if give:
        for step in range(1, segs):
            @pl.when(is_end)
            def _():
                pl.semaphore_signal(
                    barrier, inc=1, device_id={"bank": helper, "seg": lax.rem(my_seg + step, segs)},
                    device_id_type=MESH,
                )

    inputs = [
        pltpu.make_async_copy(source, target, input_sem.at[i])
        for i, (source, target) in enumerate(
            [(strain_hbm.at[part(chunk)], strain_ref.at[part(chunk)]) for chunk in range(chunks)]
            + [(tpl_hbm, tpl_ref)]
        )
    ]
    for load in inputs:
        load.start()
    loads = [
        pltpu.make_async_copy(source, target, table_sem.at[i])
        for i, (source, target) in enumerate(
            ((first_hbm, first), (odd_hbm, odd), (turn_hbm, turn), (last_hbm, last))
        )
    ]
    for load in loads:
        load.start()
    pl.semaphore_wait(barrier, has_left.astype(jnp.int32) + has_right.astype(jnp.int32) + segs - 1 + helps.astype(jnp.int32) * (segs - 1))

    def move(source, origin, chunk, step):
        sems = right_sem if step > 0 else left_sem
        return pltpu.make_async_remote_copy(
            src_ref=source,
            dst_ref=held.at[origin, part(chunk)],
            send_sem=sems.at[origin, chunk],
            recv_sem=recv_sem.at[origin, chunk],
            device_id={"bank": me + step},
            device_id_type=MESH,
        )

    for chunk in range(chunks):
        inputs[chunk].wait()

        @pl.when(wanted(me + 1, chunk))
        def _():
            move(strain_ref.at[part(chunk)], me, chunk, 1).start()

        @pl.when(wanted(me - 1, chunk))
        def _():
            move(strain_ref.at[part(chunk)], me, chunk, -1).start()

    held[me] = strain_ref[...]

    for load in inputs[chunks:]:
        load.wait()
    position = lax.broadcasted_iota(jnp.int32, (2 * rows, LANES), 0) // 2 * LANES
    position = position + lax.broadcasted_iota(jnp.int32, (2 * rows, LANES), 1)
    keep = position < lax.shift_right_logical(jnp.full((1, 1), rows * LANES, jnp.int32), bins_ref[...])
    value = jnp.where(keep, tpl_ref[...].astype(jnp.float32), 0.0)
    if give:
        masked[...] = value.astype(jnp.bfloat16)

    def prepare(interleaved, re_ref, im_ref):
        work[...] = interleaved
        re_ref[...] = work[pl.ds(0, rows, stride=2), :]
        im_ref[...] = work[pl.ds(1, rows, stride=2), :]
        return jnp.sqrt(jnp.sum(interleaved * interleaved, keepdims=True) + EPSILON)

    sigma = prepare(value, tpl_re, tpl_im)

    def lend():
        return pltpu.make_async_remote_copy(
            src_ref=masked, dst_ref=lent, send_sem=tpl_send.at[0], recv_sem=tpl_recv.at[0],
            device_id={"bank": helper}, device_id_type=MESH,
        )

    if give:
        @pl.when(is_end)
        def _():
            lend().start()

    for load in loads:
        load.wait()

    def peak(seg, re_ref, im_ref):
        work[...] = held[:, seg].reshape(2 * rows, LANES).astype(jnp.float32)
        s_re = work[pl.ds(0, rows, stride=2), :]
        s_im = work[pl.ds(1, rows, stride=2), :]
        h_re, h_im = re_ref[...], im_ref[...]
        q_re = h_re * s_re + h_im * s_im
        q_im = h_re * s_im - h_im * s_re
        even_re, even_im = q_re[:half] + q_re[half:], q_im[:half] + q_im[half:]
        d_re, d_im = q_re[:half] - q_re[half:], q_im[:half] - q_im[half:]
        odd_re = d_re * odd[0] - d_im * odd[1]
        odd_im = d_re * odd[1] + d_im * odd[0]
        y = jnp.concatenate(
            [
                jnp.concatenate([even_re, odd_re], axis=1),
                jnp.concatenate([even_im, odd_im], axis=1),
            ],
            axis=0,
        )
        high, low = split(y)
        u = jnp.dot(
            first[...],
            jnp.concatenate([high, low, high], axis=0),
            preferred_element_type=jnp.float32,
        )
        u_re, u_im = u[:half], u[half:]
        v_re = u_re * turn[0] - u_im * turn[1]
        v_im = u_re * turn[1] + u_im * turn[0]
        x = jnp.concatenate(
            [
                jnp.concatenate([v_re[:, :LANES], v_im[:, :LANES]], axis=1),
                jnp.concatenate([v_re[:, LANES:], v_im[:, LANES:]], axis=1),
            ],
            axis=0,
        )
        high, low = split(x)
        z = jnp.dot(
            jnp.concatenate([high, low, high], axis=1),
            last[...],
            preferred_element_type=jnp.float32,
        )
        z_re, z_im = z[:, :LANES], z[:, LANES:]
        power = z_re * z_re + z_im * z_im
        return jnp.max(power, keepdims=True)

    lane = lax.broadcasted_iota(jnp.int32, (8, LANES), 1)
    line = lax.broadcasted_iota(jnp.int32, (8, LANES), 0)
    row_bank[me] = jnp.zeros((8, LANES), jnp.float32)

    def note(seg, which, snr):
        row_bank[me] = jnp.where((lane == seg) & (line == which), snr, row_bank[me])

    for distance in range(1, banks):
        for chunk in range(chunks):
            for step in (1, -1):
                origin = me - step * distance
                inside = (origin >= 0) & (origin < banks) & wanted(me, chunk)

                @pl.when(inside)
                def _():
                    block = held.at[origin, part(chunk)]
                    move(block, origin, chunk, step).wait_recv()

                    @pl.when(wanted(me + step, chunk))
                    def _():
                        move(block, origin, chunk, step).start()

            if distance == banks - 1:
                for seg in range(chunk * size, (chunk + 1) * size):
                    if chunk < chunks - give:
                        note(seg, 0, jnp.sqrt(peak(seg, tpl_re, tpl_im)) / sigma)
                        continue

                    @pl.when(helps)
                    def _():
                        if chunk == chunks - give:
                            lend().wait_recv()
                        sigma_two = prepare(lent[...].astype(jnp.float32), two_re, two_im)
                        one = peak(seg, tpl_re, tpl_im)
                        two = peak(seg, two_re, two_im)
                        note(seg, 0, jnp.sqrt(one) / sigma)
                        note(seg, 1, jnp.sqrt(two) / sigma_two)

    row_seg[my_seg] = row_bank[me]

    def tell(buffer, axis, index, peer, send, recv):
        return pltpu.make_async_remote_copy(
            src_ref=buffer.at[index],
            dst_ref=buffer.at[index],
            send_sem=send.at[peer],
            recv_sem=recv.at[index],
            device_id={axis: peer},
            device_id_type=MESH,
        )

    def far(peer):
        return pltpu.make_async_remote_copy(
            src_ref=row_seg.at[my_seg], dst_ref=row_far.at[my_seg],
            send_sem=far_send.at[peer], recv_sem=far_recv.at[my_seg],
            device_id={"bank": helped, "seg": peer}, device_id_type=MESH,
        )

    def heard(peer):
        return pltpu.make_async_remote_copy(
            src_ref=row_seg.at[my_seg], dst_ref=row_far.at[peer],
            send_sem=far_send.at[peer], recv_sem=far_recv.at[peer],
            device_id={"bank": helper, "seg": peer}, device_id_type=MESH,
        )

    groups = (
        (row_bank, "bank", me, banks, bank_send, bank_recv),
        (row_seg, "seg", my_seg, segs, seg_send, seg_recv),
    )
    for buffer, axis, index, number, send, recv in groups:
        for step in range(1, number):
            tell(buffer, axis, index, lax.rem(index + step, number), send, recv).start()
    peers = [lax.rem(my_seg + step, segs) for step in range(1, segs)]
    if give:
        @pl.when(helps)
        def _():
            for peer in peers:
                far(peer).start()
    for chunk in range(chunks):
        for step, sems in ((1, right_sem), (-1, left_sem)):
            for distance in range(banks):
                origin = me - step * distance

                @pl.when((origin >= 0) & (origin < banks) & wanted(me + step, chunk))
                def _():
                    move(held.at[origin, part(chunk)], origin, chunk, step).wait_send()

    for buffer, axis, index, number, send, recv in reversed(groups):
        for step in range(1, number):
            other = lax.rem(index + step, number)
            tell(buffer, axis, other, other, send, recv).wait_recv()
    segment_peak = jnp.max(row_bank[...], axis=(0, 1))[None, :]
    table = row_bank[me][:1]
    template_row = jnp.max(row_seg[...], axis=0)[:1]

    def give_out(table, template_row):
        template_peak = jnp.max(template_row, axis=1, keepdims=True)
        out_ref[...] = jnp.where(line == 0, table, jnp.where(line == 1, segment_peak, template_peak))

    if give:
        @pl.when(is_end)
        def _():
            theirs = row_bank[helper][1:2]
            every = jnp.maximum(template_row, theirs)
            for peer in peers:
                heard(peer).wait_recv()
                every = jnp.maximum(every, row_far[peer][1:2])
            give_out(jnp.maximum(table, theirs), every)

        @pl.when(jnp.logical_not(is_end))
        def _():
            give_out(table, template_row)

        @pl.when(is_end)
        def _():
            lend().wait_send()

        @pl.when(helps)
        def _():
            for peer in peers:
                far(peer).wait_send()
    else:
        give_out(table, template_row)
    for buffer, axis, index, number, send, recv in groups:
        for step in range(1, number):
            tell(buffer, axis, index, lax.rem(index + step, number), send, recv).wait_send()


def unpack(out_ref, table_ref, segment_ref, template_ref):
    table_ref[...] = out_ref[0:1, : table_ref.shape[1]]
    segment_ref[...] = out_ref[1, : segment_ref.shape[0]]
    template_ref[...] = out_ref[2, :1]


def per_device(banks, segs, strain, templates, length_bins):
    count, _, width = strain.shape
    length = templates.shape[2]
    depth, rows = width // LANES, length // LANES
    chunks = count if banks <= 8 else 1
    give = 1 if banks == 4 and chunks == count > 1 else 0
    first, last, odd, turn = tables(length)
    strain = strain.reshape(count, 2, depth, LANES).transpose(0, 2, 1, 3).reshape(count, 2 * depth, LANES)
    tpl = templates.reshape(2, rows, LANES).transpose(1, 0, 2).reshape(2 * rows, LANES)
    vmem = pl.BlockSpec(memory_space=pltpu.VMEM)
    hbm = pl.BlockSpec(memory_space=pltpu.HBM)
    dma = pltpu.SemaphoreType.DMA
    out = pl.pallas_call(
        functools.partial(kernel, banks, segs, chunks, give),
        out_shape=jax.ShapeDtypeStruct((8, LANES), jnp.float32),
        in_specs=[hbm, hbm, vmem, hbm, hbm, hbm, hbm],
        out_specs=vmem,
        scratch_shapes=[
            pltpu.VMEM(strain.shape, strain.dtype),
            pltpu.VMEM(tpl.shape, tpl.dtype),
            pltpu.VMEM(tpl.shape, tpl.dtype),
            pltpu.VMEM(tpl.shape, tpl.dtype),
            pltpu.VMEM((banks, count, 2 * depth, LANES), jnp.bfloat16),
            pltpu.VMEM((rows, LANES), jnp.float32),
            pltpu.VMEM((rows, LANES), jnp.float32),
            pltpu.VMEM((rows, LANES), jnp.float32),
            pltpu.VMEM((rows, LANES), jnp.float32),
            pltpu.VMEM((2 * rows, LANES), jnp.float32),
            pltpu.VMEM(first.shape, first.dtype),
            pltpu.VMEM(last.shape, last.dtype),
            pltpu.VMEM(odd.shape, odd.dtype),
            pltpu.VMEM(turn.shape, turn.dtype),
            pltpu.VMEM((banks, 8, LANES), jnp.float32),
            pltpu.VMEM((segs, 8, LANES), jnp.float32),
            pltpu.VMEM((segs, 8, LANES), jnp.float32),
            dma((chunks + 1,)),
            dma((4,)),
            dma((banks, chunks)),
            dma((banks, chunks)),
            dma((banks, chunks)),
            dma((banks,)),
            dma((banks,)),
            dma((segs,)),
            dma((segs,)),
            dma((segs,)),
            dma((segs,)),
            dma((1,)),
            dma((1,)),
        ],
        compiler_params=pltpu.CompilerParams(collective_id=0, has_side_effects=True, vmem_limit_bytes=GRANT),
        name="search",
    )(strain, tpl, length_bins.reshape(1, 1), first, last, odd, turn)
    return pl.pallas_call(
        unpack,
        out_shape=[
            jax.ShapeDtypeStruct((1, count), jnp.float32),
            jax.ShapeDtypeStruct((count,), jnp.float32),
            jax.ShapeDtypeStruct((1,), jnp.float32),
        ],
        compiler_params=pltpu.CompilerParams(vmem_limit_bytes=1 << 20),
        in_specs=[vmem],
        out_specs=[vmem] * 3,
        name="unpack",
    )(out)


def solution(mesh):
    placed = (P(("grp", "seg"), None, "bank"), P("bank", None, None), P("bank"))
    return jax.shard_map(
        functools.partial(per_device, mesh.shape["bank"], mesh.shape["seg"]),
        mesh=mesh,
        in_specs=placed,
        out_specs=(P("bank", ("grp", "seg")), P(("grp", "seg")), P(("grp", "bank"))),
        check_vma=False,
    )
```

```python
import functools
import math

import jax
import jax.numpy as jnp
import numpy as np
from jax import lax
from jax.experimental import pallas as pl
from jax.experimental.pallas import tpu as pltpu
from jax.sharding import PartitionSpec as P

MESH = pl.DeviceIdType.MESH
EPSILON = 1e-06
LANES = 128
GRANT = 56492032


def split(value):
    high = value.astype(jnp.bfloat16)
    low = (value - high.astype(jnp.float32)).astype(jnp.bfloat16)
    return high, low


def tables(length):
    rows = length // LANES
    half = rows // 2

    def root(phase, period):
        angle = 2.0 * math.pi * (phase % period) / period
        return np.cos(angle), np.sin(angle)

    r = np.arange(half)
    c = np.arange(LANES)
    row_c, row_s = root(np.outer(r, r), half)
    first = np.block([[row_c, -row_s], [row_s, row_c]])
    col_c, col_s = root(np.outer(c, c), LANES)
    last = np.block([[col_c, col_s], [-col_s, col_c]])
    odd = np.stack([np.broadcast_to(part[:, None], (half, LANES)) for part in root(r, rows)])
    turn = [root(np.outer(2 * r + p, c), length) for p in (0, 1)]
    turn = np.stack([np.concatenate([turn[0][i], turn[1][i]], axis=1) for i in (0, 1)])

    def halves(matrix):
        high = matrix.astype(jnp.bfloat16)
        low = (matrix - high.astype(np.float64)).astype(jnp.bfloat16)
        return high, low

    f_high, f_low = halves(first)
    l_high, l_low = halves(last)
    first = np.concatenate([f_high, f_high, f_low], axis=1)
    last = np.concatenate([l_high, l_high, l_low], axis=0)
    return first, last, odd.astype(np.float32), turn.astype(np.float32)


def transform(products, first, last, odd, turn):
    half = products[0][0].shape[0] // 2
    many = len(products)
    columns = []
    for q_re, q_im in products:
        even_re, even_im = q_re[:half] + q_re[half:], q_im[:half] + q_im[half:]
        d_re, d_im = q_re[:half] - q_re[half:], q_im[:half] - q_im[half:]
        odd_re = d_re * odd[0] - d_im * odd[1]
        odd_im = d_re * odd[1] + d_im * odd[0]
        columns.append(
            jnp.concatenate(
                [jnp.concatenate([even_re, odd_re], axis=1), jnp.concatenate([even_im, odd_im], axis=1)], axis=0
            )
        )
    high, low = split(jnp.concatenate(columns, axis=1))
    u = jnp.dot(first[...], jnp.concatenate([high, low, high], axis=0), preferred_element_type=jnp.float32)
    lines = []
    for i in range(many):
        part = u[:, 2 * LANES * i : 2 * LANES * (i + 1)]
        u_re, u_im = part[:half], part[half:]
        v_re = u_re * turn[0] - u_im * turn[1]
        v_im = u_re * turn[1] + u_im * turn[0]
        lines.append(jnp.concatenate([v_re[:, :LANES], v_im[:, :LANES]], axis=1))
        lines.append(jnp.concatenate([v_re[:, LANES:], v_im[:, LANES:]], axis=1))
    high, low = split(jnp.concatenate(lines, axis=0))
    z = jnp.dot(jnp.concatenate([high, low, high], axis=1), last[...], preferred_element_type=jnp.float32)
    z_re, z_im = z[:, :LANES], z[:, LANES:]
    power = z_re * z_re + z_im * z_im
    return [jnp.max(power[2 * half * i : 2 * half * (i + 1)], keepdims=True) for i in range(many)]


def middle(
    banks, segs,
    strain_hbm, tpl_hbm, bins_ref, first_hbm, last_hbm, odd_hbm, turn_hbm,
    out_ref,
    strain_ref, tpl_ref, masked, lent, held, h_re, h_im, s_re, s_im, work, first, last, odd, turn,
    mine, near, side, across,
    strain_sem, input_sem, table_sem, end_send, own_send, pass_send, block_recv, lend_send, lend_recv,
    near_send, near_recv, side_send, side_recv, across_send, across_recv, ready,
):
    me = lax.axis_index("bank")
    my_seg = lax.axis_index("seg")
    count = strain_ref.shape[0]
    rows = tpl_ref.shape[0] // 2
    is_end = (me == 0) | (me == banks - 1)
    is_hub = jnp.logical_not(is_end)
    hub = jnp.where(me == 0, 1, banks - 2)
    other = banks - 1 - me
    end = jnp.where(me == 1, 0, banks - 1)
    far_end = banks - 1 - end
    aside = [lax.rem(my_seg + step, segs) for step in range(1, segs)]

    barrier = pltpu.get_barrier_semaphore()

    def signal(semaphore, place):
        pl.semaphore_signal(semaphore, inc=1, device_id=place, device_id_type=MESH)

    @pl.when(is_end)
    def _():
        signal(barrier, {"bank": hub})

    @pl.when(is_hub)
    def _():
        signal(barrier, {"bank": other})
        signal(barrier, {"bank": end})
        for seg in aside:
            signal(barrier, {"seg": seg})

    blocks = [
        pltpu.make_async_copy(strain_hbm.at[chunk], strain_ref.at[chunk], strain_sem.at[chunk])
        for chunk in range(count)
    ]
    template = pltpu.make_async_copy(tpl_hbm, tpl_ref, input_sem.at[0])
    loads = [
        pltpu.make_async_copy(source, target, table_sem.at[i])
        for i, (source, target) in enumerate(((first_hbm, first), (odd_hbm, odd), (turn_hbm, turn), (last_hbm, last)))
    ]
    for load in blocks + [template]:
        load.start()

    @pl.when(is_hub)
    def _():
        for load in loads:
            load.start()

    def block_copy(source, origin, chunk, to, send):
        return pltpu.make_async_remote_copy(
            src_ref=source, dst_ref=held.at[origin, chunk],
            send_sem=send.at[chunk], recv_sem=block_recv.at[origin, chunk],
            device_id={"bank": to}, device_id_type=MESH,
        )

    def lend(to):
        return pltpu.make_async_remote_copy(
            src_ref=masked, dst_ref=lent, send_sem=lend_send.at[0], recv_sem=lend_recv.at[0],
            device_id={"bank": to}, device_id_type=MESH,
        )

    def near_copy(to):
        return pltpu.make_async_remote_copy(
            src_ref=mine.at[pl.ds(0, 3)], dst_ref=near, send_sem=near_send.at[0], recv_sem=near_recv.at[0],
            device_id={"bank": to}, device_id_type=MESH,
        )

    def side_copy(row, origin, bank, to):
        return pltpu.make_async_remote_copy(
            src_ref=mine.at[row], dst_ref=side.at[origin],
            send_sem=side_send.at[row // 3, to], recv_sem=side_recv.at[origin],
            device_id={"bank": bank, "seg": to}, device_id_type=MESH,
        )

    def across_copy(which, to):
        return pltpu.make_async_remote_copy(
            src_ref=mine.at[1], dst_ref=across, send_sem=across_send.at[which], recv_sem=across_recv.at[0],
            device_id={"bank": to}, device_id_type=MESH,
        )

    def masked_template():
        value = tpl_ref[...].astype(jnp.float32)
        position = lax.broadcasted_iota(jnp.int32, value.shape, 0) // 2 * LANES
        position = position + lax.broadcasted_iota(jnp.int32, value.shape, 1)
        cutoff = lax.shift_right_logical(jnp.full((1, 1), rows * LANES, jnp.int32), bins_ref[...])
        return jnp.where(position < cutoff, value, 0.0)

    def give_out(table, segment_peak, template_peak):
        line = lax.broadcasted_iota(jnp.int32, (8, LANES), 0)
        out_ref[...] = jnp.where(line == 0, table, jnp.where(line == 1, segment_peak, template_peak))

    @pl.when(is_end)
    def _():
        template.wait()
        masked[...] = masked_template().astype(jnp.bfloat16)
        pl.semaphore_wait(barrier, 1)
        for chunk in range(count):
            blocks[chunk].wait()
            block_copy(strain_ref.at[chunk], me, chunk, hub, end_send).start()
        lend(hub).start()
        for chunk in range(count):
            block_copy(strain_ref.at[chunk], me, chunk, hub, end_send).wait_send()
        lend(hub).wait_send()
        for seg in aside:
            side_copy(2, seg, me, my_seg).wait_recv()
        near_copy(me).wait_recv()
        across_copy(0, me).wait_recv()
        template_peak = near[2]
        for seg in aside:
            template_peak = jnp.maximum(template_peak, side[seg])
        give_out(near[0], jnp.maximum(near[1], across[...]), template_peak)

    def deinterleave(value, slot):
        work[slot] = value
        return work[slot, pl.ds(0, rows, stride=2), :], work[slot, pl.ds(1, rows, stride=2), :]

    def prepare(slot, value):
        h_re[slot], h_im[slot] = deinterleave(value, 2)
        return jnp.sqrt(jnp.sum(value * value, keepdims=True) + EPSILON)

    def product(slot, seg):
        a, b, c, d = s_re[seg], s_im[seg], h_re[slot], h_im[slot]
        return c * a + d * b, c * b - d * a

    def peaks(*pairs):
        return [jnp.sqrt(power) for power in transform([product(*pair) for pair in pairs], first, last, odd, turn)]

    @pl.when(is_hub)
    def _():
        pl.semaphore_wait(barrier, 2 + len(aside))
        for chunk in range(count):
            blocks[chunk].wait()
            block_copy(strain_ref.at[chunk], me, chunk, other, own_send).start()
        for seg in aside:
            signal(ready, {"seg": seg})
        template.wait()
        sigma = prepare(0, masked_template())
        for chunk in range(count):
            held[me, chunk] = strain_ref[chunk]
        for load in loads:
            load.wait()
        for chunk in range(count):
            block = held.at[end, chunk]
            block_copy(block, end, chunk, me, pass_send).wait_recv()
            block_copy(block, end, chunk, other, pass_send).start()

        def gather(chunk):
            for origin in (other, far_end):
                block_copy(held.at[origin, chunk], origin, chunk, me, pass_send).wait_recv()
            s_re[chunk], s_im[chunk] = deinterleave(
                held[:, chunk].reshape(2 * rows, LANES).astype(jnp.float32), chunk % 2
            )

        own, theirs = {}, {}
        pairs = 2
        for start in range(0, count, pairs):
            group = range(start, min(start + pairs, count))
            for chunk in group:
                gather(chunk)
            if start == 0:
                lend(me).wait_recv()
                sigma_two = prepare(1, lent[...].astype(jnp.float32))
            for chunk in group:
                theirs[chunk], = peaks((1, chunk))
                own[chunk], = peaks((0, chunk))
        lane = lax.broadcasted_iota(jnp.int32, (1, LANES), 1)

        def row(values, scale):
            out, most = jnp.zeros((1, LANES), jnp.float32), values[0]
            for chunk in range(count):
                out = jnp.where(lane == chunk, values[chunk] / scale, out)
                most = jnp.maximum(most, values[chunk])
            return out, jnp.broadcast_to(most / scale, (1, LANES))

        own_row, own_peak = row(own, sigma)
        their_row, their_peak = row(theirs, sigma_two)
        segment_row = jnp.maximum(own_row, their_row)
        mine[0] = their_row
        mine[1] = segment_row
        mine[2] = their_peak
        mine[3] = own_peak
        pl.semaphore_wait(ready, len(aside))
        across_copy(0, far_end).start()
        for seg in aside:
            side_copy(2, my_seg, end, seg).start()
        near_copy(end).start()
        across_copy(1, other).start()
        for seg in aside:
            side_copy(3, my_seg, me, seg).start()
        for chunk in range(count):
            block_copy(strain_ref.at[chunk], me, chunk, other, own_send).wait_send()
            block_copy(held.at[end, chunk], end, chunk, other, pass_send).wait_send()
        for seg in aside:
            side_copy(3, seg, me, my_seg).wait_recv()
        across_copy(1, me).wait_recv()
        template_peak = own_peak
        for seg in aside:
            template_peak = jnp.maximum(template_peak, side[seg])
        give_out(own_row, jnp.maximum(segment_row, across[...]), template_peak)
        across_copy(0, far_end).wait_send()
        across_copy(1, other).wait_send()
        near_copy(end).wait_send()
        for seg in aside:
            side_copy(2, my_seg, end, seg).wait_send()
            side_copy(3, my_seg, me, seg).wait_send()


def line(
    banks, segs, chunks,
    strain_hbm, tpl_hbm, bins_ref, first_hbm, last_hbm, odd_hbm, turn_hbm,
    out_ref,
    strain_ref, tpl_ref, held, tpl_re, tpl_im, work, first, last, odd, turn,
    row_bank, row_seg,
    input_sem, table_sem, right_sem, left_sem, recv_sem, bank_send, bank_recv, seg_send, seg_recv,
):
    me = lax.axis_index("bank")
    my_seg = lax.axis_index("seg")
    size = strain_ref.shape[0] // chunks
    rows = tpl_ref.shape[0] // 2

    def part(chunk):
        return pl.ds(chunk * size, size)

    def exists(device):
        return (device >= 0) & (device < banks)

    barrier = pltpu.get_barrier_semaphore()
    has_left, has_right = me > 0, me < banks - 1

    @pl.when(has_left)
    def _():
        pl.semaphore_signal(barrier, inc=1, device_id={"bank": me - 1}, device_id_type=MESH)

    @pl.when(has_right)
    def _():
        pl.semaphore_signal(barrier, inc=1, device_id={"bank": me + 1}, device_id_type=MESH)

    for step in range(1, segs):
        pl.semaphore_signal(
            barrier, inc=1, device_id={"seg": lax.rem(my_seg + step, segs)}, device_id_type=MESH
        )

    inputs = [
        pltpu.make_async_copy(source, target, input_sem.at[i])
        for i, (source, target) in enumerate(
            [(strain_hbm.at[part(chunk)], strain_ref.at[part(chunk)]) for chunk in range(chunks)]
            + [(tpl_hbm, tpl_ref)]
        )
    ]
    for load in inputs:
        load.start()
    loads = [
        pltpu.make_async_copy(source, target, table_sem.at[i])
        for i, (source, target) in enumerate(
            ((first_hbm, first), (odd_hbm, odd), (turn_hbm, turn), (last_hbm, last))
        )
    ]
    for load in loads:
        load.start()
    pl.semaphore_wait(barrier, has_left.astype(jnp.int32) + has_right.astype(jnp.int32) + segs - 1)

    def move(source, origin, chunk, step):
        sems = right_sem if step > 0 else left_sem
        return pltpu.make_async_remote_copy(
            src_ref=source,
            dst_ref=held.at[origin, part(chunk)],
            send_sem=sems.at[origin, chunk],
            recv_sem=recv_sem.at[origin, chunk],
            device_id={"bank": me + step},
            device_id_type=MESH,
        )

    for chunk in range(chunks):
        inputs[chunk].wait()
        for step in (1, -1):
            @pl.when(exists(me + step))
            def _():
                move(strain_ref.at[part(chunk)], me, chunk, step).start()

    held[me] = strain_ref[...]

    for load in inputs[chunks:] + loads:
        load.wait()
    position = lax.broadcasted_iota(jnp.int32, (2 * rows, LANES), 0) // 2 * LANES
    position = position + lax.broadcasted_iota(jnp.int32, (2 * rows, LANES), 1)
    keep = position < lax.shift_right_logical(jnp.full((1, 1), rows * LANES, jnp.int32), bins_ref[...])
    value = jnp.where(keep, tpl_ref[...].astype(jnp.float32), 0.0)
    work[...] = value
    tpl_re[...] = work[pl.ds(0, rows, stride=2), :]
    tpl_im[...] = work[pl.ds(1, rows, stride=2), :]
    sigma = jnp.sqrt(jnp.sum(value * value, keepdims=True) + EPSILON)

    def snr(seg):
        work[...] = held[:, seg].reshape(2 * rows, LANES).astype(jnp.float32)
        s_re = work[pl.ds(0, rows, stride=2), :]
        s_im = work[pl.ds(1, rows, stride=2), :]
        h_re, h_im = tpl_re[...], tpl_im[...]
        power, = transform([(h_re * s_re + h_im * s_im, h_re * s_im - h_im * s_re)], first, last, odd, turn)
        return jnp.sqrt(power) / sigma

    lane = lax.broadcasted_iota(jnp.int32, (8, LANES), 1)
    row_bank[me] = jnp.zeros((8, LANES), jnp.float32)

    for distance in range(1, banks):
        for chunk in range(chunks):
            for step in (1, -1):
                origin = me - step * distance

                @pl.when(exists(origin))
                def _():
                    block = held.at[origin, part(chunk)]
                    move(block, origin, chunk, step).wait_recv()

                    @pl.when(exists(me + step))
                    def _():
                        move(block, origin, chunk, step).start()

            if distance == banks - 1:
                for seg in range(chunk * size, (chunk + 1) * size):
                    row_bank[me] = jnp.where(lane == seg, snr(seg), row_bank[me])

    row_seg[my_seg] = row_bank[me]

    def tell(buffer, axis, index, peer, send, recv):
        return pltpu.make_async_remote_copy(
            src_ref=buffer.at[index],
            dst_ref=buffer.at[index],
            send_sem=send.at[peer],
            recv_sem=recv.at[index],
            device_id={axis: peer},
            device_id_type=MESH,
        )

    groups = (
        (row_bank, "bank", me, banks, bank_send, bank_recv),
        (row_seg, "seg", my_seg, segs, seg_send, seg_recv),
    )
    for buffer, axis, index, number, send, recv in groups:
        for step in range(1, number):
            tell(buffer, axis, index, lax.rem(index + step, number), send, recv).start()
    for chunk in range(chunks):
        for step in (1, -1):
            for distance in range(banks):
                origin = me - step * distance

                @pl.when(exists(origin) & exists(me + step))
                def _():
                    move(held.at[origin, part(chunk)], origin, chunk, step).wait_send()

    for buffer, axis, index, number, send, recv in reversed(groups):
        for step in range(1, number):
            other = lax.rem(index + step, number)
            tell(buffer, axis, other, other, send, recv).wait_recv()
    segment_peak = jnp.max(row_bank[...], axis=(0, 1))[None, :]
    template_peak = jnp.max(jnp.max(row_seg[...], axis=0)[:1], axis=1, keepdims=True)
    index = lax.broadcasted_iota(jnp.int32, (8, LANES), 0)
    out_ref[...] = jnp.where(index == 0, row_bank[me][:1], jnp.where(index == 1, segment_peak, template_peak))
    for buffer, axis, index, number, send, recv in groups:
        for step in range(1, number):
            tell(buffer, axis, index, lax.rem(index + step, number), send, recv).wait_send()


def unpack(out_ref, table_ref, segment_ref, template_ref):
    table_ref[...] = out_ref[0:1, : table_ref.shape[1]]
    segment_ref[...] = out_ref[1, : segment_ref.shape[0]]
    template_ref[...] = out_ref[2, :1]


def per_device(banks, segs, strain, templates, length_bins):
    count, _, width = strain.shape
    length = templates.shape[2]
    depth, rows = width // LANES, length // LANES
    first, last, odd, turn = tables(length)
    strain = strain.reshape(count, 2, depth, LANES).transpose(0, 2, 1, 3).reshape(count, 2 * depth, LANES)
    tpl = templates.reshape(2, rows, LANES).transpose(1, 0, 2).reshape(2 * rows, LANES)
    vmem = pl.BlockSpec(memory_space=pltpu.VMEM)
    hbm = pl.BlockSpec(memory_space=pltpu.HBM)
    dma = pltpu.SemaphoreType.DMA
    bf16, f32 = jnp.bfloat16, jnp.float32
    held = pltpu.VMEM((banks, count, 2 * depth, LANES), bf16)
    constants = [pltpu.VMEM(table.shape, table.dtype) for table in (first, last, odd, turn)]
    if banks == 4 and count > 2:
        body = functools.partial(middle, banks, segs)
        scratch = [
            pltpu.VMEM(strain.shape, bf16),
            pltpu.VMEM(tpl.shape, bf16),
            pltpu.VMEM(tpl.shape, bf16),
            pltpu.VMEM(tpl.shape, bf16),
            held,
            pltpu.VMEM((2, rows, LANES), f32),
            pltpu.VMEM((2, rows, LANES), f32),
            pltpu.VMEM((count, rows, LANES), f32),
            pltpu.VMEM((count, rows, LANES), f32),
            pltpu.VMEM((3, 2 * rows, LANES), f32),
            *constants,
            pltpu.VMEM((4, 1, LANES), f32),
            pltpu.VMEM((3, 1, LANES), f32),
            pltpu.VMEM((segs, 1, LANES), f32),
            pltpu.VMEM((1, LANES), f32),
            dma((count,)),
            dma((1,)),
            dma((4,)),
            dma((count,)),
            dma((count,)),
            dma((count,)),
            dma((banks, count)),
            dma((1,)),
            dma((1,)),
            dma((1,)),
            dma((1,)),
            dma((2, segs)),
            dma((segs,)),
            dma((2,)),
            dma((1,)),
            pltpu.SemaphoreType.REGULAR,
        ]
    else:
        chunks = count if banks <= 8 else 1
        body = functools.partial(line, banks, segs, chunks)
        scratch = [
            pltpu.VMEM(strain.shape, bf16),
            pltpu.VMEM(tpl.shape, bf16),
            held,
            pltpu.VMEM((rows, LANES), f32),
            pltpu.VMEM((rows, LANES), f32),
            pltpu.VMEM((2 * rows, LANES), f32),
            *constants,
            pltpu.VMEM((banks, 8, LANES), f32),
            pltpu.VMEM((segs, 8, LANES), f32),
            dma((chunks + 1,)),
            dma((4,)),
            dma((banks, chunks)),
            dma((banks, chunks)),
            dma((banks, chunks)),
            dma((banks,)),
            dma((banks,)),
            dma((segs,)),
            dma((segs,)),
        ]
    out = pl.pallas_call(
        body,
        out_shape=jax.ShapeDtypeStruct((8, LANES), f32),
        in_specs=[hbm, hbm, vmem, hbm, hbm, hbm, hbm],
        out_specs=vmem,
        scratch_shapes=scratch,
        compiler_params=pltpu.CompilerParams(collective_id=0, has_side_effects=True, vmem_limit_bytes=GRANT),
        name="search",
    )(strain, tpl, length_bins.reshape(1, 1), first, last, odd, turn)
    return pl.pallas_call(
        unpack,
        out_shape=[
            jax.ShapeDtypeStruct((1, count), f32),
            jax.ShapeDtypeStruct((count,), f32),
            jax.ShapeDtypeStruct((1,), f32),
        ],
        compiler_params=pltpu.CompilerParams(vmem_limit_bytes=1 << 20),
        in_specs=[vmem],
        out_specs=[vmem] * 3,
        name="unpack",
    )(out)


def solution(mesh):
    placed = (P(("grp", "seg"), None, "bank"), P("bank", None, None), P("bank"))
    return jax.shard_map(
        functools.partial(per_device, mesh.shape["bank"], mesh.shape["seg"]),
        mesh=mesh,
        in_specs=placed,
        out_specs=(P("bank", ("grp", "seg")), P(("grp", "seg")), P(("grp", "bank"))),
        check_vma=False,
    )
```

```python
import functools
import math

import jax
import jax.numpy as jnp
import numpy as np
from jax import lax
from jax.experimental import pallas as pl
from jax.experimental.pallas import tpu as pltpu
from jax.sharding import PartitionSpec as P

MESH = pl.DeviceIdType.MESH
EPSILON = 1e-06
LANES = 128
WAYS = 4
PARTS = 1
GRANT = 56492032


def split(value):
    high = value.astype(jnp.bfloat16)
    low = (value - high.astype(jnp.float32)).astype(jnp.bfloat16)
    return high, low


def tables(length):
    rows = length // LANES
    depth = rows // WAYS

    def root(phase, period):
        angle = 2.0 * math.pi * (phase % period) / period
        return np.cos(angle), np.sin(angle)

    r = np.arange(depth)
    c = np.arange(LANES)
    row_c, row_s = root(np.outer(r, r), depth)
    first = np.block([[row_c, -row_s], [row_s, row_c]])
    col_c, col_s = root(np.outer(c, c), LANES)
    last = np.block([[col_c, col_s], [-col_s, col_c]])
    twist = [root(r * way, rows) for way in range(1, WAYS)]
    twist = np.stack([[np.broadcast_to(part[:, None], (depth, LANES)) for part in pair] for pair in twist])
    turn = [root(np.outer(WAYS * r + way, c), length) for way in range(WAYS)]
    turn = np.stack([np.concatenate([pair[i] for pair in turn], axis=1) for i in (0, 1)])

    def halves(matrix):
        high = matrix.astype(jnp.bfloat16)
        low = (matrix - high.astype(np.float64)).astype(jnp.bfloat16)
        return high, low

    f_high, f_low = halves(first)
    l_high, l_low = halves(last)
    first = np.concatenate([f_high, f_high, f_low], axis=1)
    last = np.concatenate([l_high, l_high, l_low], axis=0)
    return first, last, twist.astype(np.float32), turn.astype(np.float32)


def times(a, b):
    return a[0] * b[0] - a[1] * b[1], a[0] * b[1] + a[1] * b[0]


def transform(q_re, q_im, first, last, twist, turn):
    depth = q_re.shape[0] // WAYS
    (a, e), (b, f), (c, g), (d, h) = [
        (q_re[depth * i : depth * (i + 1)], q_im[depth * i : depth * (i + 1)]) for i in range(WAYS)
    ]
    p_re, p_im, m_re, m_im = a + c, e + g, a - c, e - g
    r_re, r_im, n_re, n_im = b + d, f + h, b - d, f - h
    ways = [(p_re + r_re, p_im + r_im), (m_re - n_im, m_im + n_re), (p_re - r_re, p_im - r_im), (m_re + n_im, m_im - n_re)]
    ways = ways[:1] + [times(ways[i], (twist[i - 1, 0], twist[i - 1, 1])) for i in range(1, WAYS)]
    y = jnp.concatenate([jnp.concatenate([way[i] for way in ways], axis=1) for i in (0, 1)], axis=0)
    high, low = split(y)
    u = jnp.dot(first[...], jnp.concatenate([high, low, high], axis=0), preferred_element_type=jnp.float32)
    v_re, v_im = times((u[:depth], u[depth:]), (turn[0], turn[1]))
    x = [
        jnp.concatenate([v_re[:, LANES * i : LANES * (i + 1)], v_im[:, LANES * i : LANES * (i + 1)]], axis=1)
        for i in range(WAYS)
    ]
    high, low = split(jnp.concatenate(x, axis=0))
    z = jnp.dot(jnp.concatenate([high, low, high], axis=1), last[...], preferred_element_type=jnp.float32)
    z_re, z_im = z[:, :LANES], z[:, LANES:]
    return jnp.max(z_re * z_re + z_im * z_im, keepdims=True)


def middle(
    banks, segs,
    strain_hbm, tpl_hbm, bins_ref, first_hbm, last_hbm, twist_hbm, turn_hbm,
    out_ref,
    strain_ref, tpl_ref, masked, lent, held, h_re, h_im, s_re, s_im, work, first, last, twist, turn,
    mine, near, side, across,
    strain_sem, input_sem, table_sem, end_send, own_send, pass_send, block_recv, lend_send, lend_recv, share_send,
    near_send, near_recv, side_send, side_recv, across_send, across_recv, ready,
):
    me = lax.axis_index("bank")
    my_seg = lax.axis_index("seg")
    count = strain_ref.shape[0]
    rows = tpl_ref.shape[0] // 2
    piece_rows = lent.shape[1]
    is_end = (me == 0) | (me == banks - 1)
    is_hub = jnp.logical_not(is_end)
    hub = jnp.where(me == 0, 1, banks - 2)
    other = banks - 1 - me
    end = jnp.where(me == 1, 0, banks - 1)
    far_end = banks - 1 - end
    size = strain_ref.shape[1] // PARTS
    parts = [pl.ds(i * size, size) for i in range(PARTS)]
    aside = [lax.rem(my_seg + step, segs) for step in range(1, segs)]

    barrier = pltpu.get_barrier_semaphore()

    def signal(semaphore, place):
        pl.semaphore_signal(semaphore, inc=1, device_id=place, device_id_type=MESH)

    @pl.when(is_end)
    def _():
        signal(barrier, {"bank": hub})

    @pl.when(is_hub)
    def _():
        signal(barrier, {"bank": other})
        signal(barrier, {"bank": end})
        for seg in aside:
            signal(barrier, {"seg": seg})

    blocks = [
        pltpu.make_async_copy(strain_hbm.at[chunk], strain_ref.at[chunk], strain_sem.at[chunk])
        for chunk in range(count)
    ]
    template = pltpu.make_async_copy(tpl_hbm, tpl_ref, input_sem.at[0])
    own_piece = pl.ds(my_seg * piece_rows, piece_rows)
    piece = pltpu.make_async_copy(tpl_hbm.at[own_piece], tpl_ref.at[own_piece], input_sem.at[1])
    loads = [
        pltpu.make_async_copy(source, target, table_sem.at[i])
        for i, (source, target) in enumerate(((first_hbm, first), (twist_hbm, twist), (turn_hbm, turn), (last_hbm, last)))
    ]
    @pl.when(is_end)
    def _():
        piece.start()

    for load in blocks:
        load.start()

    @pl.when(is_hub)
    def _():
        for load in [template] + loads:
            load.start()

    def block_copies(source, origin, chunk, to, send):
        return [
            pltpu.make_async_remote_copy(
                src_ref=source.at[part], dst_ref=held.at[origin, chunk, part],
                send_sem=send.at[chunk, i], recv_sem=block_recv.at[origin, chunk, i],
                device_id={"bank": to}, device_id_type=MESH,
            )
            for i, part in enumerate(parts)
        ]

    def lender(chunk):
        return {0: 0, count // 2: banks - 1}.get(chunk, -1)

    def lend(to):
        return pltpu.make_async_remote_copy(
            src_ref=masked, dst_ref=lent.at[my_seg], send_sem=lend_send.at[0], recv_sem=lend_recv.at[my_seg],
            device_id={"bank": to}, device_id_type=MESH,
        )

    def share(index, to):
        return pltpu.make_async_remote_copy(
            src_ref=lent.at[index], dst_ref=lent.at[index], send_sem=share_send.at[to], recv_sem=lend_recv.at[index],
            device_id={"seg": to}, device_id_type=MESH,
        )

    def near_copy(to):
        return pltpu.make_async_remote_copy(
            src_ref=mine.at[pl.ds(0, 3)], dst_ref=near, send_sem=near_send.at[0], recv_sem=near_recv.at[0],
            device_id={"bank": to}, device_id_type=MESH,
        )

    def side_copy(row, origin, bank, to):
        return pltpu.make_async_remote_copy(
            src_ref=mine.at[row], dst_ref=side.at[origin],
            send_sem=side_send.at[row // 3, to], recv_sem=side_recv.at[origin],
            device_id={"bank": bank, "seg": to}, device_id_type=MESH,
        )

    def across_copy(which, to):
        return pltpu.make_async_remote_copy(
            src_ref=mine.at[1], dst_ref=across, send_sem=across_send.at[which], recv_sem=across_recv.at[0],
            device_id={"bank": to}, device_id_type=MESH,
        )

    def mask(value, offset):
        value = value.astype(jnp.float32)
        position = (lax.broadcasted_iota(jnp.int32, value.shape, 0) + offset) // 2 * LANES
        position = position + lax.broadcasted_iota(jnp.int32, value.shape, 1)
        cutoff = lax.shift_right_logical(jnp.full((1, 1), rows * LANES, jnp.int32), bins_ref[...])
        return jnp.where(position < cutoff, value, 0.0)

    def give_out(table, segment_peak, template_peak):
        line = lax.broadcasted_iota(jnp.int32, (8, LANES), 0)
        out_ref[...] = jnp.where(line == 0, table, jnp.where(line == 1, segment_peak, template_peak))

    @pl.when(is_end)
    def _():
        piece.wait()
        masked[...] = mask(tpl_ref[own_piece, :], my_seg * piece_rows).astype(jnp.bfloat16)
        pl.semaphore_wait(barrier, 1)
        for chunk in range(count):
            @pl.when(me == lender(chunk))
            def _():
                lend(hub).start()

            blocks[chunk].wait()
            for copy in block_copies(strain_ref.at[chunk], me, chunk, hub, end_send):
                copy.start()
        for chunk in range(count):
            for copy in block_copies(strain_ref.at[chunk], me, chunk, hub, end_send):
                copy.wait_send()
        lend(hub).wait_send()
        for seg in aside:
            side_copy(2, seg, me, my_seg).wait_recv()
        near_copy(me).wait_recv()
        across_copy(0, me).wait_recv()
        template_peak = near[2]
        for seg in aside:
            template_peak = jnp.maximum(template_peak, side[seg])
        give_out(near[0], jnp.maximum(near[1], across[...]), template_peak)

    def deinterleave(value, slot):
        work[slot] = value
        return work[slot, pl.ds(0, rows, stride=2), :], work[slot, pl.ds(1, rows, stride=2), :]

    def prepare(slot, value):
        h_re[slot], h_im[slot] = deinterleave(value, 2)
        return jnp.sqrt(jnp.sum(value * value, keepdims=True) + EPSILON)

    def product(slot, seg):
        a, b, c, d = s_re[seg], s_im[seg], h_re[slot], h_im[slot]
        return c * a + d * b, c * b - d * a

    def peak(slot, seg):
        return jnp.sqrt(transform(*product(slot, seg), first, last, twist, turn))

    @pl.when(is_hub)
    def _():
        pl.semaphore_wait(barrier, 2 + len(aside))
        for chunk in range(count):
            blocks[chunk].wait()
            for copy in block_copies(strain_ref.at[chunk], me, chunk, other, own_send):
                copy.start()
        for seg in aside:
            signal(ready, {"seg": seg})
        template.wait()
        sigma = prepare(0, mask(tpl_ref[...], 0))
        for load in loads:
            load.wait()
        for chunk in range(count):
            held[me, chunk] = strain_ref[chunk]
        for chunk in range(count):
            @pl.when(end == lender(chunk))
            def _():
                lend(me).wait_recv()
                for seg in aside:
                    share(my_seg, seg).start()

            block = held.at[end, chunk]
            arriving = block_copies(block, end, chunk, me, pass_send)
            for copy, onward in zip(arriving, block_copies(block, end, chunk, other, pass_send)):
                copy.wait_recv()
                onward.start()

        def gather(*chunks):
            for chunk in chunks:
                for origin in (other, far_end):
                    for copy in block_copies(held.at[origin, chunk], origin, chunk, me, pass_send):
                        copy.wait_recv()
                s_re[chunk], s_im[chunk] = deinterleave(
                    held[:, chunk].reshape(2 * rows, LANES).astype(jnp.float32), chunk % 2
                )

        def borrow():
            for seg in aside:
                share(seg, my_seg).wait_recv()
            return prepare(1, lent[...].reshape(2 * rows, LANES).astype(jnp.float32))

        lane = lax.broadcasted_iota(jnp.int32, (1, LANES), 1)

        def row(values, scale):
            out, most = jnp.zeros((1, LANES), jnp.float32), values[0]
            for chunk in range(count):
                out = jnp.where(lane == chunk, values[chunk] / scale, out)
                most = jnp.maximum(most, values[chunk])
            return out, jnp.broadcast_to(most / scale, (1, LANES))

        def send_side(sigma_two):
            mine[0], mine[2] = row(theirs, sigma_two)
            pl.semaphore_wait(ready, len(aside))
            for seg in aside:
                side_copy(2, my_seg, end, seg).start()

        def send_rest():
            mine[4], mine[3] = row(own, sigma)
            mine[1] = jnp.maximum(mine[0], mine[4])
            across_copy(0, far_end).start()
            near_copy(end).start()
            across_copy(1, other).start()
            for seg in aside:
                side_copy(3, my_seg, me, seg).start()

        early, late = range(count // 2), range(count // 2, count)
        own, theirs = {}, {}

        @pl.when(me == 1)
        def _():
            sigma_two = borrow()
            gather(0)
            theirs[0] = peak(1, 0)
            own[0] = peak(0, 0)
            gather(1)
            theirs[1] = peak(1, 1)
            own[1] = peak(0, 1)
            gather(2, 3)
            theirs[2] = peak(1, 2)
            theirs[3] = peak(1, 3)
            send_side(sigma_two)
            own[2] = peak(0, 2)
            own[3] = peak(0, 3)
            send_rest()

        @pl.when(me != 1)
        def _():
            gather(0, 1)
            own[0] = peak(0, 0)
            own[1] = peak(0, 1)
            gather(2, 3)
            own[2] = peak(0, 2)
            own[3] = peak(0, 3)
            sigma_two = borrow()
            theirs[0] = peak(1, 0)
            theirs[1] = peak(1, 1)
            theirs[2] = peak(1, 2)
            theirs[3] = peak(1, 3)
            send_side(sigma_two)
            send_rest()

        for seg in aside:
            share(my_seg, seg).wait_send()
        for chunk in range(count):
            for copy in block_copies(strain_ref.at[chunk], me, chunk, other, own_send):
                copy.wait_send()
            for copy in block_copies(held.at[end, chunk], end, chunk, other, pass_send):
                copy.wait_send()
        for seg in aside:
            side_copy(3, seg, me, my_seg).wait_recv()
        across_copy(1, me).wait_recv()
        template_peak = mine[3]
        for seg in aside:
            template_peak = jnp.maximum(template_peak, side[seg])
        give_out(mine[4], jnp.maximum(mine[1], across[...]), template_peak)
        across_copy(0, far_end).wait_send()
        across_copy(1, other).wait_send()
        near_copy(end).wait_send()
        for seg in aside:
            side_copy(2, my_seg, end, seg).wait_send()
            side_copy(3, my_seg, me, seg).wait_send()


def line(
    banks, segs, chunks,
    strain_hbm, tpl_hbm, bins_ref, first_hbm, last_hbm, twist_hbm, turn_hbm,
    out_ref,
    strain_ref, tpl_ref, held, tpl_re, tpl_im, work, first, last, twist, turn,
    row_bank, row_seg,
    input_sem, table_sem, right_sem, left_sem, recv_sem, bank_send, bank_recv, seg_send, seg_recv,
):
    me = lax.axis_index("bank")
    my_seg = lax.axis_index("seg")
    size = strain_ref.shape[0] // chunks
    rows = tpl_ref.shape[0] // 2

    def part(chunk):
        return pl.ds(chunk * size, size)

    def exists(device):
        return (device >= 0) & (device < banks)

    barrier = pltpu.get_barrier_semaphore()
    has_left, has_right = me > 0, me < banks - 1

    @pl.when(has_left)
    def _():
        pl.semaphore_signal(barrier, inc=1, device_id={"bank": me - 1}, device_id_type=MESH)

    @pl.when(has_right)
    def _():
        pl.semaphore_signal(barrier, inc=1, device_id={"bank": me + 1}, device_id_type=MESH)

    for step in range(1, segs):
        pl.semaphore_signal(
            barrier, inc=1, device_id={"seg": lax.rem(my_seg + step, segs)}, device_id_type=MESH
        )

    inputs = [
        pltpu.make_async_copy(source, target, input_sem.at[i])
        for i, (source, target) in enumerate(
            [(strain_hbm.at[part(chunk)], strain_ref.at[part(chunk)]) for chunk in range(chunks)]
            + [(tpl_hbm, tpl_ref)]
        )
    ]
    for load in inputs:
        load.start()
    loads = [
        pltpu.make_async_copy(source, target, table_sem.at[i])
        for i, (source, target) in enumerate(
            ((first_hbm, first), (twist_hbm, twist), (turn_hbm, turn), (last_hbm, last))
        )
    ]
    for load in loads:
        load.start()
    pl.semaphore_wait(barrier, has_left.astype(jnp.int32) + has_right.astype(jnp.int32) + segs - 1)

    def move(source, origin, chunk, step):
        sems = right_sem if step > 0 else left_sem
        return pltpu.make_async_remote_copy(
            src_ref=source,
            dst_ref=held.at[origin, part(chunk)],
            send_sem=sems.at[origin, chunk],
            recv_sem=recv_sem.at[origin, chunk],
            device_id={"bank": me + step},
            device_id_type=MESH,
        )

    for chunk in range(chunks):
        inputs[chunk].wait()
        for step in (1, -1):
            @pl.when(exists(me + step))
            def _():
                move(strain_ref.at[part(chunk)], me, chunk, step).start()

    held[me] = strain_ref[...]

    for load in inputs[chunks:] + loads:
        load.wait()
    position = lax.broadcasted_iota(jnp.int32, (2 * rows, LANES), 0) // 2 * LANES
    position = position + lax.broadcasted_iota(jnp.int32, (2 * rows, LANES), 1)
    keep = position < lax.shift_right_logical(jnp.full((1, 1), rows * LANES, jnp.int32), bins_ref[...])
    value = jnp.where(keep, tpl_ref[...].astype(jnp.float32), 0.0)
    work[...] = value
    tpl_re[...] = work[pl.ds(0, rows, stride=2), :]
    tpl_im[...] = work[pl.ds(1, rows, stride=2), :]
    sigma = jnp.sqrt(jnp.sum(value * value, keepdims=True) + EPSILON)

    def snr(seg):
        work[...] = held[:, seg].reshape(2 * rows, LANES).astype(jnp.float32)
        s_re = work[pl.ds(0, rows, stride=2), :]
        s_im = work[pl.ds(1, rows, stride=2), :]
        h_re, h_im = tpl_re[...], tpl_im[...]
        q_re, q_im = h_re * s_re + h_im * s_im, h_re * s_im - h_im * s_re
        return jnp.sqrt(transform(q_re, q_im, first, last, twist, turn)) / sigma

    lane = lax.broadcasted_iota(jnp.int32, (8, LANES), 1)
    row_bank[me] = jnp.zeros((8, LANES), jnp.float32)

    for distance in range(1, banks):
        for chunk in range(chunks):
            for step in (1, -1):
                origin = me - step * distance

                @pl.when(exists(origin))
                def _():
                    block = held.at[origin, part(chunk)]
                    move(block, origin, chunk, step).wait_recv()

                    @pl.when(exists(me + step))
                    def _():
                        move(block, origin, chunk, step).start()

            if distance == banks - 1:
                for seg in range(chunk * size, (chunk + 1) * size):
                    row_bank[me] = jnp.where(lane == seg, snr(seg), row_bank[me])

    row_seg[my_seg] = row_bank[me]

    def tell(buffer, axis, index, peer, send, recv):
        return pltpu.make_async_remote_copy(
            src_ref=buffer.at[index],
            dst_ref=buffer.at[index],
            send_sem=send.at[peer],
            recv_sem=recv.at[index],
            device_id={axis: peer},
            device_id_type=MESH,
        )

    groups = (
        (row_bank, "bank", me, banks, bank_send, bank_recv),
        (row_seg, "seg", my_seg, segs, seg_send, seg_recv),
    )
    for buffer, axis, index, number, send, recv in groups:
        for step in range(1, number):
            tell(buffer, axis, index, lax.rem(index + step, number), send, recv).start()
    for chunk in range(chunks):
        for step in (1, -1):
            for distance in range(banks):
                origin = me - step * distance

                @pl.when(exists(origin) & exists(me + step))
                def _():
                    move(held.at[origin, part(chunk)], origin, chunk, step).wait_send()

    for buffer, axis, index, number, send, recv in reversed(groups):
        for step in range(1, number):
            other = lax.rem(index + step, number)
            tell(buffer, axis, other, other, send, recv).wait_recv()
    segment_peak = jnp.max(row_bank[...], axis=(0, 1))[None, :]
    template_peak = jnp.max(jnp.max(row_seg[...], axis=0)[:1], axis=1, keepdims=True)
    index = lax.broadcasted_iota(jnp.int32, (8, LANES), 0)
    out_ref[...] = jnp.where(index == 0, row_bank[me][:1], jnp.where(index == 1, segment_peak, template_peak))
    for buffer, axis, index, number, send, recv in groups:
        for step in range(1, number):
            tell(buffer, axis, index, lax.rem(index + step, number), send, recv).wait_send()


def unpack(out_ref, table_ref, segment_ref, template_ref):
    table_ref[...] = out_ref[0:1, : table_ref.shape[1]]
    segment_ref[...] = out_ref[1, : segment_ref.shape[0]]
    template_ref[...] = out_ref[2, :1]


def per_device(banks, segs, strain, templates, length_bins):
    count, _, width = strain.shape
    length = templates.shape[2]
    depth, rows = width // LANES, length // LANES
    first, last, twist, turn = tables(length)
    strain = strain.reshape(count, 2, depth, LANES).transpose(0, 2, 1, 3).reshape(count, 2 * depth, LANES)
    tpl = templates.reshape(2, rows, LANES).transpose(1, 0, 2).reshape(2 * rows, LANES)
    vmem = pl.BlockSpec(memory_space=pltpu.VMEM)
    hbm = pl.BlockSpec(memory_space=pltpu.HBM)
    dma = pltpu.SemaphoreType.DMA
    bf16, f32 = jnp.bfloat16, jnp.float32
    held = pltpu.VMEM((banks, count, 2 * depth, LANES), bf16)
    constants = [pltpu.VMEM(table.shape, table.dtype) for table in (first, last, twist, turn)]
    if banks == 4 and count > 2:
        body = functools.partial(middle, banks, segs)
        piece_rows = 2 * rows // segs
        scratch = [
            pltpu.VMEM(strain.shape, bf16),
            pltpu.VMEM(tpl.shape, bf16),
            pltpu.VMEM((piece_rows, LANES), bf16),
            pltpu.VMEM((segs, piece_rows, LANES), bf16),
            held,
            pltpu.VMEM((2, rows, LANES), f32),
            pltpu.VMEM((2, rows, LANES), f32),
            pltpu.VMEM((count, rows, LANES), f32),
            pltpu.VMEM((count, rows, LANES), f32),
            pltpu.VMEM((3, 2 * rows, LANES), f32),
            *constants,
            pltpu.VMEM((5, 1, LANES), f32),
            pltpu.VMEM((3, 1, LANES), f32),
            pltpu.VMEM((segs, 1, LANES), f32),
            pltpu.VMEM((1, LANES), f32),
            dma((count,)),
            dma((2,)),
            dma((4,)),
            dma((count, PARTS)),
            dma((count, PARTS)),
            dma((count, PARTS)),
            dma((banks, count, PARTS)),
            dma((1,)),
            dma((segs,)),
            dma((segs,)),
            dma((1,)),
            dma((1,)),
            dma((2, segs)),
            dma((segs,)),
            dma((2,)),
            dma((1,)),
            pltpu.SemaphoreType.REGULAR,
        ]
    else:
        chunks = count if banks <= 8 else 1
        body = functools.partial(line, banks, segs, chunks)
        scratch = [
            pltpu.VMEM(strain.shape, bf16),
            pltpu.VMEM(tpl.shape, bf16),
            held,
            pltpu.VMEM((rows, LANES), f32),
            pltpu.VMEM((rows, LANES), f32),
            pltpu.VMEM((2 * rows, LANES), f32),
            *constants,
            pltpu.VMEM((banks, 8, LANES), f32),
            pltpu.VMEM((segs, 8, LANES), f32),
            dma((chunks + 1,)),
            dma((4,)),
            dma((banks, chunks)),
            dma((banks, chunks)),
            dma((banks, chunks)),
            dma((banks,)),
            dma((banks,)),
            dma((segs,)),
            dma((segs,)),
        ]
    out = pl.pallas_call(
        body,
        out_shape=jax.ShapeDtypeStruct((8, LANES), f32),
        in_specs=[hbm, hbm, vmem, hbm, hbm, hbm, hbm],
        out_specs=vmem,
        scratch_shapes=scratch,
        compiler_params=pltpu.CompilerParams(collective_id=0, has_side_effects=True, vmem_limit_bytes=GRANT),
        name="search",
    )(strain, tpl, length_bins.reshape(1, 1), first, last, twist, turn)
    return pl.pallas_call(
        unpack,
        out_shape=[
            jax.ShapeDtypeStruct((1, count), f32),
            jax.ShapeDtypeStruct((count,), f32),
            jax.ShapeDtypeStruct((1,), f32),
        ],
        compiler_params=pltpu.CompilerParams(vmem_limit_bytes=1 << 20),
        in_specs=[vmem],
        out_specs=[vmem] * 3,
        name="unpack",
    )(out)


def solution(mesh):
    placed = (P(("grp", "seg"), None, "bank"), P("bank", None, None), P("bank"))
    return jax.shard_map(
        functools.partial(per_device, mesh.shape["bank"], mesh.shape["seg"]),
        mesh=mesh,
        in_specs=placed,
        out_specs=(P("bank", ("grp", "seg")), P(("grp", "seg")), P(("grp", "bank"))),
        check_vma=False,
    )
```

```python
import functools
import math

import jax
import jax.numpy as jnp
import numpy as np
from jax import lax
from jax.experimental import pallas as pl
from jax.experimental.pallas import tpu as pltpu
from jax.sharding import PartitionSpec as P

MESH = pl.DeviceIdType.MESH
EPSILON = 1e-06
LANES = 128
WAYS = 4
GRANT = 56492032


def split(value):
    high = value.astype(jnp.bfloat16)
    low = (value - high.astype(jnp.float32)).astype(jnp.bfloat16)
    return high, low


def tables(length):
    rows = length // LANES
    depth = rows // WAYS

    def root(phase, period):
        angle = 2.0 * math.pi * (phase % period) / period
        return np.cos(angle), np.sin(angle)

    r = np.arange(depth)
    c = np.arange(LANES)
    row_c, row_s = root(np.outer(r, r), depth)
    first = np.block([[row_c, -row_s], [row_s, row_c]])
    col_c, col_s = root(np.outer(c, c), LANES)
    last = np.block([[col_c, col_s], [-col_s, col_c]])
    twist = [root(np.outer(r * way, np.ones(LANES, int)), rows) for way in range(1, WAYS)]
    turn = [root(np.outer(WAYS * r + way, c), length) for way in range(WAYS)]
    spin = np.stack([np.stack(pair) for pair in turn + twist])

    def halves(matrix):
        high = matrix.astype(jnp.bfloat16)
        low = (matrix - high.astype(np.float64)).astype(jnp.bfloat16)
        return high, low

    f_high, f_low = halves(first)
    l_high, l_low = halves(last)
    first = np.concatenate([f_high, f_high, f_low], axis=1)
    last = np.concatenate([l_high, l_high, l_low], axis=0)
    return first, last, spin.astype(np.float32)


def times(a, b):
    return a[0] * b[0] - a[1] * b[1], a[0] * b[1] + a[1] * b[0]


def transform(q_re, q_im, first, last, spin):
    depth = q_re.shape[0] // WAYS
    (a, e), (b, f), (c, g), (d, h) = [
        (q_re[depth * i : depth * (i + 1)], q_im[depth * i : depth * (i + 1)]) for i in range(WAYS)
    ]
    p_re, p_im, m_re, m_im = a + c, e + g, a - c, e - g
    r_re, r_im, n_re, n_im = b + d, f + h, b - d, f - h
    ways = [(p_re + r_re, p_im + r_im), (m_re - n_im, m_im + n_re), (p_re - r_re, p_im - r_im), (m_re + n_im, m_im - n_re)]
    ways = ways[:1] + [times(ways[i], (spin[WAYS + i - 1, 0], spin[WAYS + i - 1, 1])) for i in range(1, WAYS)]
    y = jnp.concatenate([jnp.concatenate([way[i] for way in ways], axis=1) for i in (0, 1)], axis=0)
    high, low = split(y)
    u = jnp.dot(first[...], jnp.concatenate([high, low, high], axis=0), preferred_element_type=jnp.float32)
    x = []
    for i in range(WAYS):
        part = u[:, LANES * i : LANES * (i + 1)]
        x.append(jnp.concatenate(times((part[:depth], part[depth:]), (spin[i, 0], spin[i, 1])), axis=1))
    high, low = split(jnp.concatenate(x, axis=0))
    z = jnp.dot(jnp.concatenate([high, low, high], axis=1), last[...], preferred_element_type=jnp.float32)
    z_re, z_im = z[:, :LANES], z[:, LANES:]
    return jnp.max(z_re * z_re + z_im * z_im, keepdims=True)


def middle(
    banks, segs,
    strain_hbm, tpl_hbm, bins_ref, first_hbm, last_hbm, spin_hbm,
    out_ref,
    strain_ref, tpl_ref, masked, lent, held, h_re, h_im, s_re, s_im, work, first, last, spin,
    mine, inbox,
    strain_sem, tpl_sem, table_sem, block_send, pass_send, end_recv, other_recv, far_recv,
    lend_send, lend_recv, share_send, share_recv, row_send, row_recv, ready,
):
    me = lax.axis_index("bank")
    my_seg = lax.axis_index("seg")
    count = strain_ref.shape[0]
    rows = tpl_ref.shape[0] // 2
    piece_rows = lent.shape[1]
    is_end = (me == 0) | (me == banks - 1)
    is_hub = jnp.logical_not(is_end)
    hub = jnp.where(me == 0, 1, banks - 2)
    other = banks - 1 - me
    end = jnp.where(me == 1, 0, banks - 1)
    far_end = banks - 1 - end
    early, late = range(count // 2), range(count // 2, count)
    aside = [lax.rem(my_seg + step, segs) for step in range(1, segs)]

    barrier = pltpu.get_barrier_semaphore()

    def signal(semaphore, place):
        pl.semaphore_signal(semaphore, inc=1, device_id=place, device_id_type=MESH)

    @pl.when(is_end)
    def _():
        signal(barrier, {"bank": hub})

    @pl.when(is_hub)
    def _():
        signal(barrier, {"bank": other})
        signal(barrier, {"bank": end})
        for seg in aside:
            signal(barrier, {"seg": seg})

    own_piece = pl.ds(my_seg * piece_rows, piece_rows)
    piece = pltpu.make_async_copy(tpl_hbm.at[own_piece], tpl_ref.at[own_piece], tpl_sem)
    template = pltpu.make_async_copy(tpl_hbm, tpl_ref, tpl_sem)
    blocks = pltpu.make_async_copy(strain_hbm, strain_ref, strain_sem)
    loads = [
        pltpu.make_async_copy(source, target, table_sem.at[i])
        for i, (source, target) in enumerate(((first_hbm, first), (spin_hbm, spin), (last_hbm, last)))
    ]

    @pl.when(is_end)
    def _():
        piece.start()

    blocks.start()

    @pl.when(is_hub)
    def _():
        for load in [template] + loads:
            load.start()

    def remote(source, target, sent, arrived, place):
        return pltpu.make_async_remote_copy(
            src_ref=source, dst_ref=target, send_sem=sent, recv_sem=arrived, device_id=place, device_id_type=MESH
        )

    def from_end(origin, chunk, to):
        return remote(strain_ref.at[chunk], held.at[origin, chunk], block_send, end_recv.at[chunk], {"bank": to})

    def from_hub(origin, chunk, to):
        return remote(strain_ref.at[chunk], held.at[origin, chunk], block_send, other_recv, {"bank": to})

    def passed(origin, chunk, to):
        block = held.at[origin, chunk]
        return remote(block, block, pass_send, far_recv.at[min(chunk, late[0])], {"bank": to})

    def all_of(block, sent, arrived):
        return remote(block, block, sent, arrived, {"bank": hub})

    def lender(chunk):
        return {0: 0, late[0]: banks - 1}.get(chunk, -1)

    def lend(to):
        return remote(masked, lent.at[my_seg], lend_send, lend_recv, {"bank": to})

    def share(to):
        return remote(lent.at[my_seg], lent.at[my_seg], share_send, share_recv, {"seg": to})

    others = lent.at[pl.ds(0, segs - 1)]
    near, across, side = 0, 3, 4

    def row_copy(row, target, place, number=1):
        part = pl.ds(row, number)
        return remote(mine.at[part], inbox.at[pl.ds(target, number)], row_send, row_recv, place)

    def rows_of(number):
        return all_of(inbox.at[pl.ds(0, number)], row_send, row_recv)

    def mask(value, offset):
        value = value.astype(jnp.float32)
        position = (lax.broadcasted_iota(jnp.int32, value.shape, 0) + offset) // 2 * LANES
        position = position + lax.broadcasted_iota(jnp.int32, value.shape, 1)
        cutoff = lax.shift_right_logical(jnp.full((1, 1), rows * LANES, jnp.int32), bins_ref[...])
        return jnp.where(position < cutoff, value, 0.0)

    def give_out(table, segment_peak, template_peak):
        for seg in aside:
            template_peak = jnp.maximum(template_peak, inbox[side + seg])
        line = lax.broadcasted_iota(jnp.int32, (8, LANES), 0)
        segment_peak = jnp.maximum(segment_peak, inbox[across])
        out_ref[...] = jnp.where(line == 0, table, jnp.where(line == 1, segment_peak, template_peak))

    @pl.when(is_end)
    def _():
        piece.wait()
        masked[...] = mask(tpl_ref[own_piece, :], my_seg * piece_rows).astype(jnp.bfloat16)
        pl.semaphore_wait(barrier, 1)
        blocks.wait()
        for chunk in range(count):
            @pl.when(me == lender(chunk))
            def _():
                lend(hub).start()

            from_end(me, chunk, hub).start()
        all_of(strain_ref, block_send, other_recv).wait_send()
        lend(hub).wait_send()
        rows_of(4 + len(aside)).wait_recv()
        give_out(inbox[near], inbox[near + 1], inbox[near + 2])

    def deinterleave(value, slot):
        work[slot] = value
        return work[slot, pl.ds(0, rows, stride=2), :], work[slot, pl.ds(1, rows, stride=2), :]

    def prepare(slot, value):
        h_re[slot], h_im[slot] = deinterleave(value, 2)
        return jnp.sqrt(jnp.sum(value * value, keepdims=True) + EPSILON)

    def peak(slot, seg):
        a, b, c, d = s_re[seg], s_im[seg], h_re[slot], h_im[slot]
        return jnp.sqrt(transform(c * a + d * b, c * b - d * a, first, last, spin))

    @pl.when(is_hub)
    def _():
        pl.semaphore_wait(barrier, 2 + len(aside))
        blocks.wait()
        for chunk in range(count):
            from_hub(me, chunk, other).start()
        for seg in aside:
            signal(ready, {"seg": seg})
        template.wait()
        sigma = prepare(0, mask(tpl_ref[...], 0))
        for load in loads:
            load.wait()
        held[me] = strain_ref[...]
        for chunk in range(count):
            @pl.when(end == lender(chunk))
            def _():
                lend(me).wait_recv()
                for seg in aside:
                    share(seg).start()

            from_end(end, chunk, me).wait_recv()
            passed(end, chunk, other).start()
        all_of(held.at[other], block_send, other_recv).wait_recv()

        def gather(*chunks):
            if len(chunks) > 1:
                all_of(held.at[far_end, pl.ds(chunks[0], len(chunks))], pass_send, far_recv.at[chunks[0]]).wait_recv()
            else:
                passed(far_end, chunks[0], me).wait_recv()
            for chunk in chunks:
                s_re[chunk], s_im[chunk] = deinterleave(
                    held[:, chunk].reshape(2 * rows, LANES).astype(jnp.float32), chunk % 2
                )

        def borrow():
            all_of(others, share_send, share_recv).wait_recv()
            return prepare(1, lent[...].reshape(2 * rows, LANES).astype(jnp.float32))

        lane = lax.broadcasted_iota(jnp.int32, (1, LANES), 1)

        def row(values, scale):
            out, most = jnp.zeros((1, LANES), jnp.float32), values[0]
            for chunk in range(count):
                out = jnp.where(lane == chunk, values[chunk] / scale, out)
                most = jnp.maximum(most, values[chunk])
            return out, jnp.broadcast_to(most / scale, (1, LANES))

        def send_side(sigma_two):
            mine[0], mine[2] = row(theirs, sigma_two)
            pl.semaphore_wait(ready, len(aside))
            for seg in aside:
                row_copy(2, side + my_seg, {"bank": end, "seg": seg}).start()

        def send_rest():
            mine[4], mine[3] = row(own, sigma)
            mine[1] = jnp.maximum(mine[0], mine[4])
            row_copy(1, across, {"bank": far_end}).start()
            row_copy(0, near, {"bank": end}, 3).start()
            row_copy(1, across, {"bank": other}).start()
            for seg in aside:
                row_copy(3, side + my_seg, {"seg": seg}).start()

        own, theirs = {}, {}

        @pl.when(me == 1)
        def _():
            sigma_two = borrow()
            for chunk in early:
                gather(chunk)
                theirs[chunk] = peak(1, chunk)
                own[chunk] = peak(0, chunk)
            gather(*late)
            for chunk in late:
                theirs[chunk] = peak(1, chunk)
            send_side(sigma_two)
            for chunk in late:
                own[chunk] = peak(0, chunk)
            send_rest()

        @pl.when(me != 1)
        def _():
            for chunk in early:
                gather(chunk)
            for chunk in early:
                own[chunk] = peak(0, chunk)
            gather(*late)
            for chunk in late:
                own[chunk] = peak(0, chunk)
            sigma_two = borrow()
            for chunk in range(count):
                theirs[chunk] = peak(1, chunk)
            send_side(sigma_two)
            send_rest()

        all_of(others, share_send, share_recv).wait_send()
        all_of(strain_ref, block_send, other_recv).wait_send()
        all_of(held.at[end], pass_send, other_recv).wait_send()
        rows_of(1 + len(aside)).wait_recv()
        give_out(mine[4], mine[1], mine[3])
        rows_of(5 + 2 * len(aside)).wait_send()


def line(
    banks, segs, chunks,
    strain_hbm, tpl_hbm, bins_ref, first_hbm, last_hbm, spin_hbm,
    out_ref,
    strain_ref, tpl_ref, held, tpl_re, tpl_im, work, first, last, spin,
    row_bank, row_seg,
    input_sem, table_sem, right_sem, left_sem, recv_sem, bank_send, bank_recv, seg_send, seg_recv,
):
    me = lax.axis_index("bank")
    my_seg = lax.axis_index("seg")
    size = strain_ref.shape[0] // chunks
    rows = tpl_ref.shape[0] // 2

    def part(chunk):
        return pl.ds(chunk * size, size)

    def exists(device):
        return (device >= 0) & (device < banks)

    barrier = pltpu.get_barrier_semaphore()
    has_left, has_right = me > 0, me < banks - 1

    @pl.when(has_left)
    def _():
        pl.semaphore_signal(barrier, inc=1, device_id={"bank": me - 1}, device_id_type=MESH)

    @pl.when(has_right)
    def _():
        pl.semaphore_signal(barrier, inc=1, device_id={"bank": me + 1}, device_id_type=MESH)

    for step in range(1, segs):
        pl.semaphore_signal(
            barrier, inc=1, device_id={"seg": lax.rem(my_seg + step, segs)}, device_id_type=MESH
        )

    inputs = [
        pltpu.make_async_copy(source, target, input_sem.at[i])
        for i, (source, target) in enumerate(
            [(strain_hbm.at[part(chunk)], strain_ref.at[part(chunk)]) for chunk in range(chunks)]
            + [(tpl_hbm, tpl_ref)]
        )
    ]
    for load in inputs:
        load.start()
    loads = [
        pltpu.make_async_copy(source, target, table_sem.at[i])
        for i, (source, target) in enumerate(
            ((first_hbm, first), (spin_hbm, spin), (last_hbm, last))
        )
    ]
    for load in loads:
        load.start()
    pl.semaphore_wait(barrier, has_left.astype(jnp.int32) + has_right.astype(jnp.int32) + segs - 1)

    def move(source, origin, chunk, step):
        sems = right_sem if step > 0 else left_sem
        return pltpu.make_async_remote_copy(
            src_ref=source,
            dst_ref=held.at[origin, part(chunk)],
            send_sem=sems.at[origin, chunk],
            recv_sem=recv_sem.at[origin, chunk],
            device_id={"bank": me + step},
            device_id_type=MESH,
        )

    for chunk in range(chunks):
        inputs[chunk].wait()
        for step in (1, -1):
            @pl.when(exists(me + step))
            def _():
                move(strain_ref.at[part(chunk)], me, chunk, step).start()

    held[me] = strain_ref[...]

    for load in inputs[chunks:] + loads:
        load.wait()
    position = lax.broadcasted_iota(jnp.int32, (2 * rows, LANES), 0) // 2 * LANES
    position = position + lax.broadcasted_iota(jnp.int32, (2 * rows, LANES), 1)
    keep = position < lax.shift_right_logical(jnp.full((1, 1), rows * LANES, jnp.int32), bins_ref[...])
    value = jnp.where(keep, tpl_ref[...].astype(jnp.float32), 0.0)
    work[...] = value
    tpl_re[...] = work[pl.ds(0, rows, stride=2), :]
    tpl_im[...] = work[pl.ds(1, rows, stride=2), :]
    sigma = jnp.sqrt(jnp.sum(value * value, keepdims=True) + EPSILON)

    def snr(seg):
        work[...] = held[:, seg].reshape(2 * rows, LANES).astype(jnp.float32)
        s_re = work[pl.ds(0, rows, stride=2), :]
        s_im = work[pl.ds(1, rows, stride=2), :]
        h_re, h_im = tpl_re[...], tpl_im[...]
        q_re, q_im = h_re * s_re + h_im * s_im, h_re * s_im - h_im * s_re
        return jnp.sqrt(transform(q_re, q_im, first, last, spin)) / sigma

    lane = lax.broadcasted_iota(jnp.int32, (8, LANES), 1)
    row_bank[me] = jnp.zeros((8, LANES), jnp.float32)

    for distance in range(1, banks):
        for chunk in range(chunks):
            for step in (1, -1):
                origin = me - step * distance

                @pl.when(exists(origin))
                def _():
                    block = held.at[origin, part(chunk)]
                    move(block, origin, chunk, step).wait_recv()

                    @pl.when(exists(me + step))
                    def _():
                        move(block, origin, chunk, step).start()

            if distance == banks - 1:
                for seg in range(chunk * size, (chunk + 1) * size):
                    row_bank[me] = jnp.where(lane == seg, snr(seg), row_bank[me])

    row_seg[my_seg] = row_bank[me]

    def tell(buffer, axis, index, peer, send, recv):
        return pltpu.make_async_remote_copy(
            src_ref=buffer.at[index],
            dst_ref=buffer.at[index],
            send_sem=send.at[peer],
            recv_sem=recv.at[index],
            device_id={axis: peer},
            device_id_type=MESH,
        )

    groups = (
        (row_bank, "bank", me, banks, bank_send, bank_recv),
        (row_seg, "seg", my_seg, segs, seg_send, seg_recv),
    )
    for buffer, axis, index, number, send, recv in groups:
        for step in range(1, number):
            tell(buffer, axis, index, lax.rem(index + step, number), send, recv).start()
    for chunk in range(chunks):
        for step in (1, -1):
            for distance in range(banks):
                origin = me - step * distance

                @pl.when(exists(origin) & exists(me + step))
                def _():
                    move(held.at[origin, part(chunk)], origin, chunk, step).wait_send()

    for buffer, axis, index, number, send, recv in reversed(groups):
        for step in range(1, number):
            other = lax.rem(index + step, number)
            tell(buffer, axis, other, other, send, recv).wait_recv()
    segment_peak = jnp.max(row_bank[...], axis=(0, 1))[None, :]
    template_peak = jnp.max(jnp.max(row_seg[...], axis=0)[:1], axis=1, keepdims=True)
    index = lax.broadcasted_iota(jnp.int32, (8, LANES), 0)
    out_ref[...] = jnp.where(index == 0, row_bank[me][:1], jnp.where(index == 1, segment_peak, template_peak))
    for buffer, axis, index, number, send, recv in groups:
        for step in range(1, number):
            tell(buffer, axis, index, lax.rem(index + step, number), send, recv).wait_send()


def unpack(out_ref, table_ref, segment_ref, template_ref):
    table_ref[...] = out_ref[0:1, : table_ref.shape[1]]
    segment_ref[...] = out_ref[1, : segment_ref.shape[0]]
    template_ref[...] = out_ref[2, :1]


def per_device(banks, segs, strain, templates, length_bins):
    count, _, width = strain.shape
    length = templates.shape[2]
    depth, rows = width // LANES, length // LANES
    first, last, spin = tables(length)
    strain = strain.reshape(count, 2, depth, LANES).transpose(0, 2, 1, 3).reshape(count, 2 * depth, LANES)
    tpl = templates.reshape(2, rows, LANES).transpose(1, 0, 2).reshape(2 * rows, LANES)
    vmem = pl.BlockSpec(memory_space=pltpu.VMEM)
    hbm = pl.BlockSpec(memory_space=pltpu.HBM)
    dma = pltpu.SemaphoreType.DMA
    bf16, f32 = jnp.bfloat16, jnp.float32
    held = pltpu.VMEM((banks, count, 2 * depth, LANES), bf16)
    constants = [pltpu.VMEM(table.shape, table.dtype) for table in (first, last, spin)]
    if banks == 4 and count > 2:
        body = functools.partial(middle, banks, segs)
        piece_rows = 2 * rows // segs
        scratch = [
            pltpu.VMEM(strain.shape, bf16),
            pltpu.VMEM(tpl.shape, bf16),
            pltpu.VMEM((piece_rows, LANES), bf16),
            pltpu.VMEM((segs, piece_rows, LANES), bf16),
            held,
            pltpu.VMEM((2, rows, LANES), f32),
            pltpu.VMEM((2, rows, LANES), f32),
            pltpu.VMEM((count, rows, LANES), f32),
            pltpu.VMEM((count, rows, LANES), f32),
            pltpu.VMEM((3, 2 * rows, LANES), f32),
            *constants,
            pltpu.VMEM((5, 1, LANES), f32),
            pltpu.VMEM((max(4, segs + 1) + 2 * segs, 1, LANES), f32),
            dma,
            dma,
            dma((3,)),
            dma,
            dma,
            dma((count,)),
            dma,
            dma((count // 2 + 1,)),
            dma,
            dma,
            dma,
            dma,
            dma,
            dma,
            pltpu.SemaphoreType.REGULAR,
        ]
    else:
        chunks = count if banks <= 8 else 1
        body = functools.partial(line, banks, segs, chunks)
        scratch = [
            pltpu.VMEM(strain.shape, bf16),
            pltpu.VMEM(tpl.shape, bf16),
            held,
            pltpu.VMEM((rows, LANES), f32),
            pltpu.VMEM((rows, LANES), f32),
            pltpu.VMEM((2 * rows, LANES), f32),
            *constants,
            pltpu.VMEM((banks, 8, LANES), f32),
            pltpu.VMEM((segs, 8, LANES), f32),
            dma((chunks + 1,)),
            dma((3,)),
            dma((banks, chunks)),
            dma((banks, chunks)),
            dma((banks, chunks)),
            dma((banks,)),
            dma((banks,)),
            dma((segs,)),
            dma((segs,)),
        ]
    out = pl.pallas_call(
        body,
        out_shape=jax.ShapeDtypeStruct((8, LANES), f32),
        in_specs=[hbm, hbm, vmem, hbm, hbm, hbm],
        out_specs=vmem,
        scratch_shapes=scratch,
        compiler_params=pltpu.CompilerParams(collective_id=0, has_side_effects=True, vmem_limit_bytes=GRANT),
        name="search",
    )(strain, tpl, length_bins.reshape(1, 1), first, last, spin)
    return pl.pallas_call(
        unpack,
        out_shape=[
            jax.ShapeDtypeStruct((1, count), f32),
            jax.ShapeDtypeStruct((count,), f32),
            jax.ShapeDtypeStruct((1,), f32),
        ],
        compiler_params=pltpu.CompilerParams(vmem_limit_bytes=1 << 20),
        in_specs=[vmem],
        out_specs=[vmem] * 3,
        name="unpack",
    )(out)


def solution(mesh):
    placed = (P(("grp", "seg"), None, "bank"), P("bank", None, None), P("bank"))
    return jax.shard_map(
        functools.partial(per_device, mesh.shape["bank"], mesh.shape["seg"]),
        mesh=mesh,
        in_specs=placed,
        out_specs=(P("bank", ("grp", "seg")), P(("grp", "seg")), P(("grp", "bank"))),
        check_vma=False,
    )
```

```python
import functools
import math

import jax
import jax.numpy as jnp
import numpy as np
from jax import lax
from jax.experimental import pallas as pl
from jax.experimental.pallas import tpu as pltpu
from jax.sharding import PartitionSpec as P

MESH = pl.DeviceIdType.MESH
EPSILON = 1e-06
LANES = 128
WAYS = 4
GRANT = 56492032


def split(value):
    high = value.astype(jnp.bfloat16)
    low = (value - high.astype(jnp.float32)).astype(jnp.bfloat16)
    return high, low


def tables(length):
    rows = length // LANES
    depth = rows // WAYS

    def root(phase, period):
        angle = 2.0 * math.pi * (phase % period) / period
        return np.cos(angle), np.sin(angle)

    r = np.arange(depth)
    c = np.arange(LANES)
    row_c, row_s = root(np.outer(r, r), depth)
    first = np.block([[row_c, -row_s], [row_s, row_c]])
    col_c, col_s = root(np.outer(c, c), LANES)
    last = np.block([[col_c, col_s], [-col_s, col_c]])
    twist = [root(np.outer(r * way, np.ones(LANES, int)), rows) for way in range(1, WAYS)]
    turn = [root(np.outer(WAYS * r + way, c), length) for way in range(WAYS)]
    spin = np.stack([np.stack(pair) for pair in turn + twist])

    def halves(matrix):
        high = matrix.astype(jnp.bfloat16)
        low = (matrix - high.astype(np.float64)).astype(jnp.bfloat16)
        return high, low

    f_high, f_low = halves(first)
    l_high, l_low = halves(last)
    first = np.concatenate([f_high, f_high, f_low], axis=1)
    last = np.concatenate([l_high, l_high, l_low], axis=0)
    return first, last, spin.astype(np.float32)


def times(a, b):
    return a[0] * b[0] - a[1] * b[1], a[0] * b[1] + a[1] * b[0]


def butterfly(parts):
    number = len(parts)
    if number == 1:
        return parts
    evens, odds = butterfly(parts[0::2]), butterfly(parts[1::2])
    root = math.sqrt(0.5)
    out = [None] * number
    for way, ((a, b), (c, d)) in enumerate(zip(evens, odds)):
        if 4 * way == number:
            c, d = -d, c
        elif 8 * way == number:
            c, d = (c - d) * root, (c + d) * root
        elif 8 * way == 3 * number:
            c, d = (c + d) * -root, (c - d) * root
        out[way], out[way + number // 2] = (a + c, b + d), (a - c, b - d)
    return out


def transform(q_re, q_im, first, last, spin):
    depth = q_re.shape[0] // WAYS
    ways = butterfly(
        [(q_re[depth * i : depth * (i + 1)], q_im[depth * i : depth * (i + 1)]) for i in range(WAYS)]
    )
    ways = ways[:1] + [times(ways[i], (spin[WAYS + i - 1, 0], spin[WAYS + i - 1, 1])) for i in range(1, WAYS)]
    y = jnp.concatenate([jnp.concatenate([way[i] for way in ways], axis=1) for i in (0, 1)], axis=0)
    high, low = split(y)
    u = jnp.dot(first[...], jnp.concatenate([high, low, high], axis=0), preferred_element_type=jnp.float32)
    x = []
    for i in range(WAYS):
        part = u[:, LANES * i : LANES * (i + 1)]
        x.append(jnp.concatenate(times((part[:depth], part[depth:]), (spin[i, 0], spin[i, 1])), axis=1))
    high, low = split(jnp.concatenate(x, axis=0))
    z = jnp.dot(jnp.concatenate([high, low, high], axis=1), last[...], preferred_element_type=jnp.float32)
    z_re, z_im = z[:, :LANES], z[:, LANES:]
    return jnp.max(z_re * z_re + z_im * z_im, keepdims=True)


def middle(
    banks, segs,
    strain_hbm, tpl_hbm, bins_ref, first_hbm, last_hbm, spin_hbm,
    out_ref,
    strain_ref, tpl_ref, masked, lent, held, h_re, h_im, s_re, s_im, work, first, last, spin,
    mine, inbox,
    strain_sem, tpl_sem, table_sem, block_send, pass_send, end_recv, other_recv, far_recv,
    lend_send, lend_recv, share_send, share_recv, row_send, row_recv, ready,
):
    me = lax.axis_index("bank")
    my_seg = lax.axis_index("seg")
    count = strain_ref.shape[0]
    rows = tpl_ref.shape[0] // 2
    depth = strain_ref.shape[1] // 2
    piece_rows = lent.shape[1]
    is_end = (me == 0) | (me == banks - 1)
    is_hub = jnp.logical_not(is_end)
    hub = jnp.where(me == 0, 1, banks - 2)
    other = banks - 1 - me
    end = jnp.where(me == 1, 0, banks - 1)
    far_end = banks - 1 - end
    early, late = range(count // 2), range(count // 2, count)
    aside = [lax.rem(my_seg + step, segs) for step in range(1, segs)]

    barrier = pltpu.get_barrier_semaphore()

    def signal(semaphore, place):
        pl.semaphore_signal(semaphore, inc=1, device_id=place, device_id_type=MESH)

    @pl.when(is_end)
    def _():
        signal(barrier, {"bank": hub})

    @pl.when(is_hub)
    def _():
        signal(barrier, {"bank": other})
        signal(barrier, {"bank": end})
        for seg in aside:
            signal(barrier, {"seg": seg})

    own_piece = pl.ds(my_seg * piece_rows, piece_rows)
    piece = pltpu.make_async_copy(tpl_hbm.at[own_piece], tpl_ref.at[own_piece], tpl_sem)
    template = pltpu.make_async_copy(tpl_hbm, tpl_ref, tpl_sem)
    blocks = pltpu.make_async_copy(strain_hbm, strain_ref, strain_sem)
    loads = [
        pltpu.make_async_copy(source, target, table_sem.at[i])
        for i, (source, target) in enumerate(((first_hbm, first), (spin_hbm, spin), (last_hbm, last)))
    ]

    @pl.when(is_end)
    def _():
        piece.start()

    blocks.start()

    @pl.when(is_hub)
    def _():
        for load in [template] + loads:
            load.start()

    def remote(source, target, sent, arrived, place):
        return pltpu.make_async_remote_copy(
            src_ref=source, dst_ref=target, send_sem=sent, recv_sem=arrived, device_id=place, device_id_type=MESH
        )

    def from_end(origin, chunk, to):
        return remote(strain_ref.at[chunk], held.at[origin, chunk], block_send, end_recv.at[chunk], {"bank": to})

    def from_hub(origin, chunk, to):
        return remote(strain_ref.at[chunk], held.at[origin, chunk], block_send, other_recv, {"bank": to})

    def passed(origin, chunk, to):
        block = held.at[origin, chunk]
        return remote(block, block, pass_send, far_recv.at[min(chunk, late[0])], {"bank": to})

    def all_of(block, sent, arrived):
        return remote(block, block, sent, arrived, {"bank": hub})

    def lender(chunk):
        return {0: 0, late[0]: banks - 1}.get(chunk, -1)

    def lend(to):
        return remote(masked, lent.at[my_seg], lend_send, lend_recv, {"bank": to})

    def share(to):
        return remote(lent.at[my_seg], lent.at[my_seg], share_send, share_recv, {"seg": to})

    others = lent.at[pl.ds(0, segs - 1)]
    near, across, side = 0, 3, 4

    def row_copy(row, target, place, number=1):
        part = pl.ds(row, number)
        return remote(mine.at[part], inbox.at[pl.ds(target, number)], row_send, row_recv, place)

    def rows_of(number):
        return all_of(inbox.at[pl.ds(0, number)], row_send, row_recv)

    def mask(value, offset):
        value = value.astype(jnp.float32)
        position = (lax.broadcasted_iota(jnp.int32, value.shape, 0) + offset) // 2 * LANES
        position = position + lax.broadcasted_iota(jnp.int32, value.shape, 1)
        cutoff = lax.shift_right_logical(jnp.full((1, 1), rows * LANES, jnp.int32), bins_ref[...])
        return jnp.where(position < cutoff, value, 0.0)

    def give_out(table, segment_peak, template_peak):
        for seg in aside:
            template_peak = jnp.maximum(template_peak, inbox[side + seg])
        line = lax.broadcasted_iota(jnp.int32, (8, LANES), 0)
        segment_peak = jnp.maximum(segment_peak, inbox[across])
        out_ref[...] = jnp.where(line == 0, table, jnp.where(line == 1, segment_peak, template_peak))

    @pl.when(is_end)
    def _():
        piece.wait()
        masked[...] = mask(tpl_ref[own_piece, :], my_seg * piece_rows).astype(jnp.bfloat16)
        pl.semaphore_wait(barrier, 1)
        blocks.wait()
        for chunk in range(count):
            @pl.when(me == lender(chunk))
            def _():
                lend(hub).start()

            from_end(me, chunk, hub).start()
        all_of(strain_ref, block_send, other_recv).wait_send()
        lend(hub).wait_send()
        rows_of(4 + len(aside)).wait_recv()
        give_out(inbox[near], inbox[near + 1], inbox[near + 2])

    def place(block, origin, chunk):
        spare = work.at[2 + chunk]
        spare[pl.ds(origin * (2 * depth), 2 * depth), :] = block.astype(jnp.float32)
        part = pl.ds(pl.multiple_of(origin * depth, depth), depth)
        for i, target in enumerate((s_re, s_im)):
            target[chunk, part, :] = spare[pl.ds(origin * (2 * depth) + i, depth, stride=2), :]

    def prepare(slot, value):
        spare = work.at[slot]
        spare[...] = value
        for i, target in enumerate((h_re, h_im)):
            target[slot] = spare[pl.ds(i, rows, stride=2), :]
        return jnp.sqrt(jnp.sum(value * value, keepdims=True) + EPSILON)

    def peak(slot, seg):
        a, b, c, d = s_re[seg], s_im[seg], h_re[slot], h_im[slot]
        return jnp.sqrt(transform(c * a + d * b, c * b - d * a, first, last, spin))

    @pl.when(is_hub)
    def _():
        pl.semaphore_wait(barrier, 2 + len(aside))
        blocks.wait()
        for chunk in range(count):
            from_hub(me, chunk, other).start()
        for seg in aside:
            signal(ready, {"seg": seg})
        template.wait()
        sigma = prepare(0, mask(tpl_ref[...], 0))
        for load in loads:
            load.wait()
        for chunk in range(count):
            @pl.when(end == lender(chunk))
            def _():
                lend(me).wait_recv()
                for seg in aside:
                    share(seg).start()

            from_end(end, chunk, me).wait_recv()
            passed(end, chunk, other).start()
        all_of(held.at[other], block_send, other_recv).wait_recv()

        for chunk in range(count):
            place(strain_ref[chunk], me, chunk)
            for origin in (end, other):
                place(held[origin, chunk], origin, chunk)

        def gather(*chunks):
            if len(chunks) > 1:
                all_of(held.at[far_end, pl.ds(chunks[0], len(chunks))], pass_send, far_recv.at[chunks[0]]).wait_recv()
            else:
                passed(far_end, chunks[0], me).wait_recv()
            for chunk in chunks:
                place(held[far_end, chunk], far_end, chunk)

        def borrow():
            all_of(others, share_send, share_recv).wait_recv()
            return prepare(1, lent[...].reshape(2 * rows, LANES).astype(jnp.float32))

        lane = lax.broadcasted_iota(jnp.int32, (1, LANES), 1)

        def row(values, scale):
            out, most = jnp.zeros((1, LANES), jnp.float32), values[0]
            for chunk in range(count):
                out = jnp.where(lane == chunk, values[chunk] / scale, out)
                most = jnp.maximum(most, values[chunk])
            return out, jnp.broadcast_to(most / scale, (1, LANES))

        def send_side(sigma_two):
            mine[0], mine[2] = row(theirs, sigma_two)
            pl.semaphore_wait(ready, len(aside))
            for seg in aside:
                row_copy(2, side + my_seg, {"bank": end, "seg": seg}).start()

        def send_rest():
            mine[4], mine[3] = row(own, sigma)
            mine[1] = jnp.maximum(mine[0], mine[4])
            row_copy(1, across, {"bank": far_end}).start()
            row_copy(0, near, {"bank": end}, 3).start()
            row_copy(1, across, {"bank": other}).start()
            for seg in aside:
                row_copy(3, side + my_seg, {"seg": seg}).start()

        own, theirs = {}, {}

        @pl.when(me == 1)
        def _():
            sigma_two = borrow()
            for chunk in early:
                gather(chunk)
                theirs[chunk] = peak(1, chunk)
                own[chunk] = peak(0, chunk)
            gather(*late)
            for chunk in late:
                theirs[chunk] = peak(1, chunk)
            send_side(sigma_two)
            for chunk in late:
                own[chunk] = peak(0, chunk)
            send_rest()

        @pl.when(me != 1)
        def _():
            for chunk in early:
                gather(chunk)
            for chunk in early:
                own[chunk] = peak(0, chunk)
            gather(*late)
            for chunk in late:
                own[chunk] = peak(0, chunk)
            sigma_two = borrow()
            for chunk in range(count):
                theirs[chunk] = peak(1, chunk)
            send_side(sigma_two)
            send_rest()

        all_of(others, share_send, share_recv).wait_send()
        all_of(strain_ref, block_send, other_recv).wait_send()
        all_of(held.at[end], pass_send, other_recv).wait_send()
        rows_of(1 + len(aside)).wait_recv()
        give_out(mine[4], mine[1], mine[3])
        rows_of(5 + 2 * len(aside)).wait_send()


def line(
    banks, segs, chunks,
    strain_hbm, tpl_hbm, bins_ref, first_hbm, last_hbm, spin_hbm,
    out_ref,
    strain_ref, tpl_ref, held, tpl_re, tpl_im, work, first, last, spin,
    row_bank, row_seg,
    input_sem, table_sem, right_sem, left_sem, recv_sem, bank_send, bank_recv, seg_send, seg_recv,
):
    me = lax.axis_index("bank")
    my_seg = lax.axis_index("seg")
    size = strain_ref.shape[0] // chunks
    rows = tpl_ref.shape[0] // 2

    def part(chunk):
        return pl.ds(chunk * size, size)

    def exists(device):
        return (device >= 0) & (device < banks)

    barrier = pltpu.get_barrier_semaphore()
    has_left, has_right = me > 0, me < banks - 1

    @pl.when(has_left)
    def _():
        pl.semaphore_signal(barrier, inc=1, device_id={"bank": me - 1}, device_id_type=MESH)

    @pl.when(has_right)
    def _():
        pl.semaphore_signal(barrier, inc=1, device_id={"bank": me + 1}, device_id_type=MESH)

    for step in range(1, segs):
        pl.semaphore_signal(
            barrier, inc=1, device_id={"seg": lax.rem(my_seg + step, segs)}, device_id_type=MESH
        )

    inputs = [
        pltpu.make_async_copy(source, target, input_sem.at[i])
        for i, (source, target) in enumerate(
            [(strain_hbm.at[part(chunk)], strain_ref.at[part(chunk)]) for chunk in range(chunks)]
            + [(tpl_hbm, tpl_ref)]
        )
    ]
    for load in inputs:
        load.start()
    loads = [
        pltpu.make_async_copy(source, target, table_sem.at[i])
        for i, (source, target) in enumerate(
            ((first_hbm, first), (spin_hbm, spin), (last_hbm, last))
        )
    ]
    for load in loads:
        load.start()
    pl.semaphore_wait(barrier, has_left.astype(jnp.int32) + has_right.astype(jnp.int32) + segs - 1)

    def move(source, origin, chunk, step):
        sems = right_sem if step > 0 else left_sem
        return pltpu.make_async_remote_copy(
            src_ref=source,
            dst_ref=held.at[origin, part(chunk)],
            send_sem=sems.at[origin, chunk],
            recv_sem=recv_sem.at[origin, chunk],
            device_id={"bank": me + step},
            device_id_type=MESH,
        )

    for chunk in range(chunks):
        inputs[chunk].wait()
        for step in (1, -1):
            @pl.when(exists(me + step))
            def _():
                move(strain_ref.at[part(chunk)], me, chunk, step).start()

    held[me] = strain_ref[...]

    for load in inputs[chunks:] + loads:
        load.wait()
    position = lax.broadcasted_iota(jnp.int32, (2 * rows, LANES), 0) // 2 * LANES
    position = position + lax.broadcasted_iota(jnp.int32, (2 * rows, LANES), 1)
    keep = position < lax.shift_right_logical(jnp.full((1, 1), rows * LANES, jnp.int32), bins_ref[...])
    value = jnp.where(keep, tpl_ref[...].astype(jnp.float32), 0.0)
    work[...] = value
    tpl_re[...] = work[pl.ds(0, rows, stride=2), :]
    tpl_im[...] = work[pl.ds(1, rows, stride=2), :]
    sigma = jnp.sqrt(jnp.sum(value * value, keepdims=True) + EPSILON)

    def snr(seg):
        work[...] = held[:, seg].reshape(2 * rows, LANES).astype(jnp.float32)
        s_re = work[pl.ds(0, rows, stride=2), :]
        s_im = work[pl.ds(1, rows, stride=2), :]
        h_re, h_im = tpl_re[...], tpl_im[...]
        q_re, q_im = h_re * s_re + h_im * s_im, h_re * s_im - h_im * s_re
        return jnp.sqrt(transform(q_re, q_im, first, last, spin)) / sigma

    lane = lax.broadcasted_iota(jnp.int32, (8, LANES), 1)
    row_bank[me] = jnp.zeros((8, LANES), jnp.float32)

    for distance in range(1, banks):
        for chunk in range(chunks):
            for step in (1, -1):
                origin = me - step * distance

                @pl.when(exists(origin))
                def _():
                    block = held.at[origin, part(chunk)]
                    move(block, origin, chunk, step).wait_recv()

                    @pl.when(exists(me + step))
                    def _():
                        move(block, origin, chunk, step).start()

            if distance == banks - 1:
                for seg in range(chunk * size, (chunk + 1) * size):
                    row_bank[me] = jnp.where(lane == seg, snr(seg), row_bank[me])

    row_seg[my_seg] = row_bank[me]

    def tell(buffer, axis, index, peer, send, recv):
        return pltpu.make_async_remote_copy(
            src_ref=buffer.at[index],
            dst_ref=buffer.at[index],
            send_sem=send.at[peer],
            recv_sem=recv.at[index],
            device_id={axis: peer},
            device_id_type=MESH,
        )

    groups = (
        (row_bank, "bank", me, banks, bank_send, bank_recv),
        (row_seg, "seg", my_seg, segs, seg_send, seg_recv),
    )
    for buffer, axis, index, number, send, recv in groups:
        for step in range(1, number):
            tell(buffer, axis, index, lax.rem(index + step, number), send, recv).start()
    for chunk in range(chunks):
        for step in (1, -1):
            for distance in range(banks):
                origin = me - step * distance

                @pl.when(exists(origin) & exists(me + step))
                def _():
                    move(held.at[origin, part(chunk)], origin, chunk, step).wait_send()

    for buffer, axis, index, number, send, recv in reversed(groups):
        for step in range(1, number):
            other = lax.rem(index + step, number)
            tell(buffer, axis, other, other, send, recv).wait_recv()
    segment_peak = jnp.max(row_bank[...], axis=(0, 1))[None, :]
    template_peak = jnp.max(jnp.max(row_seg[...], axis=0)[:1], axis=1, keepdims=True)
    index = lax.broadcasted_iota(jnp.int32, (8, LANES), 0)
    out_ref[...] = jnp.where(index == 0, row_bank[me][:1], jnp.where(index == 1, segment_peak, template_peak))
    for buffer, axis, index, number, send, recv in groups:
        for step in range(1, number):
            tell(buffer, axis, index, lax.rem(index + step, number), send, recv).wait_send()


def unpack(out_ref, table_ref, segment_ref, template_ref):
    table_ref[...] = out_ref[0:1, : table_ref.shape[1]]
    segment_ref[...] = out_ref[1, : segment_ref.shape[0]]
    template_ref[...] = out_ref[2, :1]


def per_device(banks, segs, strain, templates, length_bins):
    count, _, width = strain.shape
    length = templates.shape[2]
    depth, rows = width // LANES, length // LANES
    first, last, spin = tables(length)
    strain = strain.reshape(count, 2, depth, LANES).transpose(0, 2, 1, 3).reshape(count, 2 * depth, LANES)
    tpl = templates.reshape(2, rows, LANES).transpose(1, 0, 2).reshape(2 * rows, LANES)
    vmem = pl.BlockSpec(memory_space=pltpu.VMEM)
    hbm = pl.BlockSpec(memory_space=pltpu.HBM)
    dma = pltpu.SemaphoreType.DMA
    bf16, f32 = jnp.bfloat16, jnp.float32
    held = pltpu.VMEM((banks, count, 2 * depth, LANES), bf16)
    constants = [pltpu.VMEM(table.shape, table.dtype) for table in (first, last, spin)]
    if banks == 4 and count > 2:
        body = functools.partial(middle, banks, segs)
        piece_rows = 2 * rows // segs
        scratch = [
            pltpu.VMEM(strain.shape, bf16),
            pltpu.VMEM(tpl.shape, bf16),
            pltpu.VMEM((piece_rows, LANES), bf16),
            pltpu.VMEM((segs, piece_rows, LANES), bf16),
            held,
            pltpu.VMEM((2, rows, LANES), f32),
            pltpu.VMEM((2, rows, LANES), f32),
            pltpu.VMEM((count, rows, LANES), f32),
            pltpu.VMEM((count, rows, LANES), f32),
            pltpu.VMEM((2 + count, 2 * rows, LANES), f32),
            *constants,
            pltpu.VMEM((5, 1, LANES), f32),
            pltpu.VMEM((max(4, segs + 1) + 2 * segs, 1, LANES), f32),
            dma,
            dma,
            dma((3,)),
            dma,
            dma,
            dma((count,)),
            dma,
            dma((count // 2 + 1,)),
            dma,
            dma,
            dma,
            dma,
            dma,
            dma,
            pltpu.SemaphoreType.REGULAR,
        ]
    else:
        chunks = count if banks <= 8 else 1
        body = functools.partial(line, banks, segs, chunks)
        scratch = [
            pltpu.VMEM(strain.shape, bf16),
            pltpu.VMEM(tpl.shape, bf16),
            held,
            pltpu.VMEM((rows, LANES), f32),
            pltpu.VMEM((rows, LANES), f32),
            pltpu.VMEM((2 * rows, LANES), f32),
            *constants,
            pltpu.VMEM((banks, 8, LANES), f32),
            pltpu.VMEM((segs, 8, LANES), f32),
            dma((chunks + 1,)),
            dma((3,)),
            dma((banks, chunks)),
            dma((banks, chunks)),
            dma((banks, chunks)),
            dma((banks,)),
            dma((banks,)),
            dma((segs,)),
            dma((segs,)),
        ]
    out = pl.pallas_call(
        body,
        out_shape=jax.ShapeDtypeStruct((8, LANES), f32),
        in_specs=[hbm, hbm, vmem, hbm, hbm, hbm],
        out_specs=vmem,
        scratch_shapes=scratch,
        compiler_params=pltpu.CompilerParams(collective_id=0, has_side_effects=True, vmem_limit_bytes=GRANT),
        name="search",
    )(strain, tpl, length_bins.reshape(1, 1), first, last, spin)
    return pl.pallas_call(
        unpack,
        out_shape=[
            jax.ShapeDtypeStruct((1, count), f32),
            jax.ShapeDtypeStruct((count,), f32),
            jax.ShapeDtypeStruct((1,), f32),
        ],
        compiler_params=pltpu.CompilerParams(vmem_limit_bytes=1 << 20),
        in_specs=[vmem],
        out_specs=[vmem] * 3,
        name="unpack",
    )(out)


def solution(mesh):
    placed = (P(("grp", "seg"), None, "bank"), P("bank", None, None), P("bank"))
    return jax.shard_map(
        functools.partial(per_device, mesh.shape["bank"], mesh.shape["seg"]),
        mesh=mesh,
        in_specs=placed,
        out_specs=(P("bank", ("grp", "seg")), P(("grp", "seg")), P(("grp", "bank"))),
        check_vma=False,
    )
```

```python
import functools
import math

import jax
import jax.numpy as jnp
import numpy as np
from jax import lax
from jax.experimental import pallas as pl
from jax.experimental.pallas import tpu as pltpu
from jax.sharding import PartitionSpec as P

MESH = pl.DeviceIdType.MESH
EPSILON = 1e-06
LANES = 128
WAYS = 8
GRANT = 56549376


def split(value):
    high = value.astype(jnp.bfloat16)
    low = (value - high.astype(jnp.float32)).astype(jnp.bfloat16)
    return high, low


def tables(length):
    rows = length // LANES
    depth = rows // WAYS

    def root(phase, period):
        angle = 2.0 * math.pi * (phase % period) / period
        return np.cos(angle), np.sin(angle)

    r = np.arange(depth)
    c = np.arange(LANES)
    row_c, row_s = root(np.outer(r, r), depth)
    first = np.block([[row_c, -row_s], [row_s, row_c]])
    col_c, col_s = root(np.outer(c, c), LANES)
    last = np.block([[col_c, col_s], [-col_s, col_c]])
    twist = [root(np.outer(r * way, np.ones(LANES, int)), rows) for way in range(1, WAYS)]
    turn = [root(np.outer(WAYS * r + way, c), length) for way in range(WAYS)]
    spin = np.stack([np.stack(pair) for pair in turn + twist])

    def halves(matrix):
        high = matrix.astype(jnp.bfloat16)
        low = (matrix - high.astype(np.float64)).astype(jnp.bfloat16)
        return high, low

    f_high, f_low = halves(first)
    l_high, l_low = halves(last)
    first = np.concatenate([f_high, f_high, f_low], axis=1)
    last = np.concatenate([l_high, l_high, l_low], axis=0)
    return first, last, spin.astype(np.float32)


def times(a, b):
    return a[0] * b[0] - a[1] * b[1], a[0] * b[1] + a[1] * b[0]


def butterfly(parts):
    number = len(parts)
    if number == 1:
        return parts
    evens, odds = butterfly(parts[0::2]), butterfly(parts[1::2])
    root = math.sqrt(0.5)
    out = [None] * number
    for way, ((a, b), (c, d)) in enumerate(zip(evens, odds)):
        if 4 * way == number:
            c, d = -d, c
        elif 8 * way == number:
            c, d = (c - d) * root, (c + d) * root
        elif 8 * way == 3 * number:
            c, d = (c + d) * -root, (c - d) * root
        out[way], out[way + number // 2] = (a + c, b + d), (a - c, b - d)
    return out


def transform(q_re, q_im, first, last, spin):
    depth = q_re.shape[0] // WAYS
    ways = butterfly(
        [(q_re[depth * i : depth * (i + 1)], q_im[depth * i : depth * (i + 1)]) for i in range(WAYS)]
    )
    ways = ways[:1] + [times(ways[i], (spin[WAYS + i - 1, 0], spin[WAYS + i - 1, 1])) for i in range(1, WAYS)]
    y = jnp.concatenate([jnp.concatenate([way[i] for way in ways], axis=1) for i in (0, 1)], axis=0)
    high, low = split(y)
    u = jnp.dot(first[...], jnp.concatenate([high, low, high], axis=0), preferred_element_type=jnp.float32)
    x = []
    for i in range(WAYS):
        part = u[:, LANES * i : LANES * (i + 1)]
        x.append(jnp.concatenate(times((part[:depth], part[depth:]), (spin[i, 0], spin[i, 1])), axis=1))
    high, low = split(jnp.concatenate(x, axis=0))
    z = jnp.dot(jnp.concatenate([high, low, high], axis=1), last[...], preferred_element_type=jnp.float32)
    z_re, z_im = z[:, :LANES], z[:, LANES:]
    return jnp.max(z_re * z_re + z_im * z_im, keepdims=True)


def middle(
    banks, segs,
    strain_hbm, tpl_hbm, bins_ref, first_hbm, last_hbm, spin_hbm,
    out_ref,
    strain_ref, tpl_ref, masked, lent, held, h_re, h_im, s_re, s_im, work, first, last, spin,
    mine, inbox,
    strain_sem, tpl_sem, table_sem, block_send, pass_send, end_recv, other_recv, far_recv,
    lend_send, lend_recv, share_send, share_recv, row_send, row_recv, ready,
):
    me = lax.axis_index("bank")
    my_seg = lax.axis_index("seg")
    count = strain_ref.shape[0]
    rows = tpl_ref.shape[0] // 2
    depth = strain_ref.shape[1] // 2
    piece_rows = lent.shape[1]
    is_end = (me == 0) | (me == banks - 1)
    is_hub = jnp.logical_not(is_end)
    hub = jnp.where(me == 0, 1, banks - 2)
    other = banks - 1 - me
    end = jnp.where(me == 1, 0, banks - 1)
    far_end = banks - 1 - end
    early, late = range(count // 2), range(count // 2, count)
    aside = [lax.rem(my_seg + step, segs) for step in range(1, segs)]

    barrier = pltpu.get_barrier_semaphore()

    def signal(semaphore, place):
        pl.semaphore_signal(semaphore, inc=1, device_id=place, device_id_type=MESH)

    @pl.when(is_end)
    def _():
        signal(barrier, {"bank": hub})

    @pl.when(is_hub)
    def _():
        signal(barrier, {"bank": other})
        signal(barrier, {"bank": end})
        for seg in aside:
            signal(barrier, {"seg": seg})

    own_piece = pl.ds(my_seg * piece_rows, piece_rows)
    piece = pltpu.make_async_copy(tpl_hbm.at[own_piece], tpl_ref.at[own_piece], tpl_sem)
    template = pltpu.make_async_copy(tpl_hbm, tpl_ref, tpl_sem)
    blocks = pltpu.make_async_copy(strain_hbm, strain_ref, strain_sem)
    loads = [
        pltpu.make_async_copy(source, target, table_sem.at[i])
        for i, (source, target) in enumerate(((first_hbm, first), (spin_hbm, spin), (last_hbm, last)))
    ]

    @pl.when(is_end)
    def _():
        piece.start()

    blocks.start()

    @pl.when(is_hub)
    def _():
        for load in [template] + loads:
            load.start()

    def remote(source, target, sent, arrived, place):
        return pltpu.make_async_remote_copy(
            src_ref=source, dst_ref=target, send_sem=sent, recv_sem=arrived, device_id=place, device_id_type=MESH
        )

    def from_end(origin, chunk, to):
        return remote(strain_ref.at[chunk], held.at[origin, chunk], block_send, end_recv.at[chunk], {"bank": to})

    def from_hub(origin, chunk, to):
        return remote(strain_ref.at[chunk], held.at[origin, chunk], block_send, other_recv, {"bank": to})

    def passed(origin, chunk, to):
        block = held.at[origin, chunk]
        return remote(block, block, pass_send, far_recv.at[min(chunk, late[0])], {"bank": to})

    def all_of(block, sent, arrived):
        return remote(block, block, sent, arrived, {"bank": hub})

    def lender(chunk):
        return {0: 0, late[0]: banks - 1}.get(chunk, -1)

    def lend(to):
        return remote(masked, lent.at[my_seg], lend_send, lend_recv, {"bank": to})

    def share(to):
        return remote(lent.at[my_seg], lent.at[my_seg], share_send, share_recv, {"seg": to})

    others = lent.at[pl.ds(0, segs - 1)]
    near, across, side = 0, 3, 4

    def row_copy(row, target, place, number=1):
        part = pl.ds(row, number)
        return remote(mine.at[part], inbox.at[pl.ds(target, number)], row_send, row_recv, place)

    def rows_of(number):
        return all_of(inbox.at[pl.ds(0, number)], row_send, row_recv)

    def mask(value, offset):
        value = value.astype(jnp.float32)
        position = (lax.broadcasted_iota(jnp.int32, value.shape, 0) + offset) // 2 * LANES
        position = position + lax.broadcasted_iota(jnp.int32, value.shape, 1)
        cutoff = lax.shift_right_logical(jnp.full((1, 1), rows * LANES, jnp.int32), bins_ref[...])
        return jnp.where(position < cutoff, value, 0.0)

    def give_out(table, segment_peak, template_peak):
        for seg in aside:
            template_peak = jnp.maximum(template_peak, inbox[side + seg])
        line = lax.broadcasted_iota(jnp.int32, (8, LANES), 0)
        segment_peak = jnp.maximum(segment_peak, inbox[across])
        out_ref[...] = jnp.where(line == 0, table, jnp.where(line == 1, segment_peak, template_peak))

    @pl.when(is_end)
    def _():
        piece.wait()
        masked[...] = mask(tpl_ref[own_piece, :], my_seg * piece_rows).astype(jnp.bfloat16)
        pl.semaphore_wait(barrier, 1)
        blocks.wait()
        for chunk in range(count):
            @pl.when(me == lender(chunk))
            def _():
                lend(hub).start()

            from_end(me, chunk, hub).start()
        all_of(strain_ref, block_send, other_recv).wait_send()
        lend(hub).wait_send()
        rows_of(4 + len(aside)).wait_recv()
        give_out(inbox[near], inbox[near + 1], inbox[near + 2])

    def place(block, origin, chunk):
        spare = work.at[2 + chunk]
        spare[pl.ds(origin * (2 * depth), 2 * depth), :] = block.astype(jnp.float32)
        part = pl.ds(pl.multiple_of(origin * depth, depth), depth)
        for i, target in enumerate((s_re, s_im)):
            target[chunk, part, :] = spare[pl.ds(origin * (2 * depth) + i, depth, stride=2), :]

    def prepare(slot, value):
        spare = work.at[slot]
        spare[...] = value
        for i, target in enumerate((h_re, h_im)):
            target[slot] = spare[pl.ds(i, rows, stride=2), :]
        return jnp.sqrt(jnp.sum(value * value, keepdims=True) + EPSILON)

    def peak(slot, seg):
        a, b, c, d = s_re[seg], s_im[seg], h_re[slot], h_im[slot]
        return transform(c * a + d * b, c * b - d * a, first, last, spin)

    @pl.when(is_hub)
    def _():
        pl.semaphore_wait(barrier, 2 + len(aside))
        blocks.wait()
        for chunk in range(count):
            from_hub(me, chunk, other).start()
        for seg in aside:
            signal(ready, {"seg": seg})
        template.wait()
        sigma = prepare(0, mask(tpl_ref[...], 0))
        for load in loads:
            load.wait()
        for chunk in range(count):
            @pl.when(end == lender(chunk))
            def _():
                lend(me).wait_recv()
                for seg in aside:
                    share(seg).start()

            from_end(end, chunk, me).wait_recv()
            passed(end, chunk, other).start()
        all_of(held.at[other], block_send, other_recv).wait_recv()

        for chunk in range(count):
            place(strain_ref[chunk], me, chunk)
            for origin in (end, other):
                place(held[origin, chunk], origin, chunk)

        def gather(*chunks):
            if len(chunks) > 1:
                all_of(held.at[far_end, pl.ds(chunks[0], len(chunks))], pass_send, far_recv.at[chunks[0]]).wait_recv()
            else:
                passed(far_end, chunks[0], me).wait_recv()
            for chunk in chunks:
                place(held[far_end, chunk], far_end, chunk)

        def borrow():
            all_of(others, share_send, share_recv).wait_recv()
            return prepare(1, lent[...].reshape(2 * rows, LANES).astype(jnp.float32))

        lane = lax.broadcasted_iota(jnp.int32, (1, LANES), 1)

        def row(values, scale):
            out, most = jnp.zeros((1, LANES), jnp.float32), values[0]
            for chunk in range(count):
                out = jnp.where(lane == chunk, values[chunk], out)
                most = jnp.maximum(most, values[chunk])
            return jnp.sqrt(out) / scale, jnp.sqrt(jnp.broadcast_to(most, (1, LANES))) / scale

        def send_side(sigma_two):
            mine[0], mine[2] = row(theirs, sigma_two)
            pl.semaphore_wait(ready, len(aside))
            for seg in aside:
                row_copy(2, side + my_seg, {"bank": end, "seg": seg}).start()

        def send_rest():
            mine[4], mine[3] = row(own, sigma)
            mine[1] = jnp.maximum(mine[0], mine[4])
            row_copy(1, across, {"bank": far_end}).start()
            row_copy(0, near, {"bank": end}, 3).start()
            row_copy(1, across, {"bank": other}).start()
            for seg in aside:
                row_copy(3, side + my_seg, {"seg": seg}).start()

        own, theirs = {}, {}

        @pl.when(me == 1)
        def _():
            sigma_two = borrow()
            for chunk in early:
                gather(chunk)
                theirs[chunk] = peak(1, chunk)
                own[chunk] = peak(0, chunk)
            gather(*late)
            for chunk in late:
                theirs[chunk] = peak(1, chunk)
            send_side(sigma_two)
            for chunk in late:
                own[chunk] = peak(0, chunk)
            send_rest()

        @pl.when(me != 1)
        def _():
            for chunk in early:
                gather(chunk)
            for chunk in early:
                own[chunk] = peak(0, chunk)
            gather(*late)
            for chunk in late:
                own[chunk] = peak(0, chunk)
            sigma_two = borrow()
            for chunk in range(count):
                theirs[chunk] = peak(1, chunk)
            send_side(sigma_two)
            send_rest()

        all_of(others, share_send, share_recv).wait_send()
        all_of(strain_ref, block_send, other_recv).wait_send()
        all_of(held.at[end], pass_send, other_recv).wait_send()
        rows_of(1 + len(aside)).wait_recv()
        give_out(mine[4], mine[1], mine[3])
        rows_of(5 + 2 * len(aside)).wait_send()


def line(
    banks, segs, chunks,
    strain_hbm, tpl_hbm, bins_ref, first_hbm, last_hbm, spin_hbm,
    out_ref,
    strain_ref, tpl_ref, held, tpl_re, tpl_im, work, first, last, spin,
    row_bank, row_seg,
    input_sem, table_sem, right_sem, left_sem, recv_sem, bank_send, bank_recv, seg_send, seg_recv,
):
    me = lax.axis_index("bank")
    my_seg = lax.axis_index("seg")
    size = strain_ref.shape[0] // chunks
    rows = tpl_ref.shape[0] // 2

    def part(chunk):
        return pl.ds(chunk * size, size)

    def exists(device):
        return (device >= 0) & (device < banks)

    barrier = pltpu.get_barrier_semaphore()
    has_left, has_right = me > 0, me < banks - 1

    @pl.when(has_left)
    def _():
        pl.semaphore_signal(barrier, inc=1, device_id={"bank": me - 1}, device_id_type=MESH)

    @pl.when(has_right)
    def _():
        pl.semaphore_signal(barrier, inc=1, device_id={"bank": me + 1}, device_id_type=MESH)

    for step in range(1, segs):
        pl.semaphore_signal(
            barrier, inc=1, device_id={"seg": lax.rem(my_seg + step, segs)}, device_id_type=MESH
        )

    inputs = [
        pltpu.make_async_copy(source, target, input_sem.at[i])
        for i, (source, target) in enumerate(
            [(strain_hbm.at[part(chunk)], strain_ref.at[part(chunk)]) for chunk in range(chunks)]
            + [(tpl_hbm, tpl_ref)]
        )
    ]
    for load in inputs:
        load.start()
    loads = [
        pltpu.make_async_copy(source, target, table_sem.at[i])
        for i, (source, target) in enumerate(
            ((first_hbm, first), (spin_hbm, spin), (last_hbm, last))
        )
    ]
    for load in loads:
        load.start()
    pl.semaphore_wait(barrier, has_left.astype(jnp.int32) + has_right.astype(jnp.int32) + segs - 1)

    def move(source, origin, chunk, step):
        sems = right_sem if step > 0 else left_sem
        return pltpu.make_async_remote_copy(
            src_ref=source,
            dst_ref=held.at[origin, part(chunk)],
            send_sem=sems.at[origin, chunk],
            recv_sem=recv_sem.at[origin, chunk],
            device_id={"bank": me + step},
            device_id_type=MESH,
        )

    for chunk in range(chunks):
        inputs[chunk].wait()
        for step in (1, -1):
            @pl.when(exists(me + step))
            def _():
                move(strain_ref.at[part(chunk)], me, chunk, step).start()

    held[me] = strain_ref[...]

    for load in inputs[chunks:] + loads:
        load.wait()
    position = lax.broadcasted_iota(jnp.int32, (2 * rows, LANES), 0) // 2 * LANES
    position = position + lax.broadcasted_iota(jnp.int32, (2 * rows, LANES), 1)
    keep = position < lax.shift_right_logical(jnp.full((1, 1), rows * LANES, jnp.int32), bins_ref[...])
    value = jnp.where(keep, tpl_ref[...].astype(jnp.float32), 0.0)
    work[...] = value
    tpl_re[...] = work[pl.ds(0, rows, stride=2), :]
    tpl_im[...] = work[pl.ds(1, rows, stride=2), :]
    sigma = jnp.sqrt(jnp.sum(value * value, keepdims=True) + EPSILON)

    def snr(seg):
        work[...] = held[:, seg].reshape(2 * rows, LANES).astype(jnp.float32)
        s_re = work[pl.ds(0, rows, stride=2), :]
        s_im = work[pl.ds(1, rows, stride=2), :]
        h_re, h_im = tpl_re[...], tpl_im[...]
        q_re, q_im = h_re * s_re + h_im * s_im, h_re * s_im - h_im * s_re
        return jnp.sqrt(transform(q_re, q_im, first, last, spin)) / sigma

    lane = lax.broadcasted_iota(jnp.int32, (8, LANES), 1)
    row_bank[me] = jnp.zeros((8, LANES), jnp.float32)

    for distance in range(1, banks):
        for chunk in range(chunks):
            for step in (1, -1):
                origin = me - step * distance

                @pl.when(exists(origin))
                def _():
                    block = held.at[origin, part(chunk)]
                    move(block, origin, chunk, step).wait_recv()

                    @pl.when(exists(me + step))
                    def _():
                        move(block, origin, chunk, step).start()

            if distance == banks - 1:
                for seg in range(chunk * size, (chunk + 1) * size):
                    row_bank[me] = jnp.where(lane == seg, snr(seg), row_bank[me])

    row_seg[my_seg] = row_bank[me]

    def tell(buffer, axis, index, peer, send, recv):
        return pltpu.make_async_remote_copy(
            src_ref=buffer.at[index],
            dst_ref=buffer.at[index],
            send_sem=send.at[peer],
            recv_sem=recv.at[index],
            device_id={axis: peer},
            device_id_type=MESH,
        )

    groups = (
        (row_bank, "bank", me, banks, bank_send, bank_recv),
        (row_seg, "seg", my_seg, segs, seg_send, seg_recv),
    )
    for buffer, axis, index, number, send, recv in groups:
        for step in range(1, number):
            tell(buffer, axis, index, lax.rem(index + step, number), send, recv).start()
    for chunk in range(chunks):
        for step in (1, -1):
            for distance in range(banks):
                origin = me - step * distance

                @pl.when(exists(origin) & exists(me + step))
                def _():
                    move(held.at[origin, part(chunk)], origin, chunk, step).wait_send()

    for buffer, axis, index, number, send, recv in reversed(groups):
        for step in range(1, number):
            other = lax.rem(index + step, number)
            tell(buffer, axis, other, other, send, recv).wait_recv()
    segment_peak = jnp.max(row_bank[...], axis=(0, 1))[None, :]
    template_peak = jnp.max(jnp.max(row_seg[...], axis=0)[:1], axis=1, keepdims=True)
    index = lax.broadcasted_iota(jnp.int32, (8, LANES), 0)
    out_ref[...] = jnp.where(index == 0, row_bank[me][:1], jnp.where(index == 1, segment_peak, template_peak))
    for buffer, axis, index, number, send, recv in groups:
        for step in range(1, number):
            tell(buffer, axis, index, lax.rem(index + step, number), send, recv).wait_send()


def unpack(out_ref, table_ref, segment_ref, template_ref):
    table_ref[...] = out_ref[0:1, : table_ref.shape[1]]
    segment_ref[...] = out_ref[1, : segment_ref.shape[0]]
    template_ref[...] = out_ref[2, :1]


def per_device(banks, segs, strain, templates, length_bins):
    count, _, width = strain.shape
    length = templates.shape[2]
    depth, rows = width // LANES, length // LANES
    first, last, spin = tables(length)
    strain = strain.reshape(count, 2, depth, LANES).transpose(0, 2, 1, 3).reshape(count, 2 * depth, LANES)
    tpl = templates.reshape(2, rows, LANES).transpose(1, 0, 2).reshape(2 * rows, LANES)
    vmem = pl.BlockSpec(memory_space=pltpu.VMEM)
    hbm = pl.BlockSpec(memory_space=pltpu.HBM)
    dma = pltpu.SemaphoreType.DMA
    bf16, f32 = jnp.bfloat16, jnp.float32
    held = pltpu.VMEM((banks, count, 2 * depth, LANES), bf16)
    constants = [pltpu.VMEM(table.shape, table.dtype) for table in (first, last, spin)]
    if banks == 4 and count > 2:
        body = functools.partial(middle, banks, segs)
        piece_rows = 2 * rows // segs
        scratch = [
            pltpu.VMEM(strain.shape, bf16),
            pltpu.VMEM(tpl.shape, bf16),
            pltpu.VMEM((piece_rows, LANES), bf16),
            pltpu.VMEM((segs, piece_rows, LANES), bf16),
            held,
            pltpu.VMEM((2, rows, LANES), f32),
            pltpu.VMEM((2, rows, LANES), f32),
            pltpu.VMEM((count, rows, LANES), f32),
            pltpu.VMEM((count, rows, LANES), f32),
            pltpu.VMEM((2 + count, 2 * rows, LANES), f32),
            *constants,
            pltpu.VMEM((5, 1, LANES), f32),
            pltpu.VMEM((max(4, segs + 1) + 2 * segs, 1, LANES), f32),
            dma,
            dma,
            dma((3,)),
            dma,
            dma,
            dma((count,)),
            dma,
            dma((count // 2 + 1,)),
            dma,
            dma,
            dma,
            dma,
            dma,
            dma,
            pltpu.SemaphoreType.REGULAR,
        ]
    else:
        chunks = count if banks <= 8 else 1
        body = functools.partial(line, banks, segs, chunks)
        scratch = [
            pltpu.VMEM(strain.shape, bf16),
            pltpu.VMEM(tpl.shape, bf16),
            held,
            pltpu.VMEM((rows, LANES), f32),
            pltpu.VMEM((rows, LANES), f32),
            pltpu.VMEM((2 * rows, LANES), f32),
            *constants,
            pltpu.VMEM((banks, 8, LANES), f32),
            pltpu.VMEM((segs, 8, LANES), f32),
            dma((chunks + 1,)),
            dma((3,)),
            dma((banks, chunks)),
            dma((banks, chunks)),
            dma((banks, chunks)),
            dma((banks,)),
            dma((banks,)),
            dma((segs,)),
            dma((segs,)),
        ]
    out = pl.pallas_call(
        body,
        out_shape=jax.ShapeDtypeStruct((8, LANES), f32),
        in_specs=[hbm, hbm, vmem, hbm, hbm, hbm],
        out_specs=vmem,
        scratch_shapes=scratch,
        compiler_params=pltpu.CompilerParams(collective_id=0, has_side_effects=True, vmem_limit_bytes=GRANT),
        name="search",
    )(strain, tpl, length_bins.reshape(1, 1), first, last, spin)
    return pl.pallas_call(
        unpack,
        out_shape=[
            jax.ShapeDtypeStruct((1, count), f32),
            jax.ShapeDtypeStruct((count,), f32),
            jax.ShapeDtypeStruct((1,), f32),
        ],
        compiler_params=pltpu.CompilerParams(vmem_limit_bytes=1 << 20),
        in_specs=[vmem],
        out_specs=[vmem] * 3,
        name="unpack",
    )(out)


def solution(mesh):
    placed = (P(("grp", "seg"), None, "bank"), P("bank", None, None), P("bank"))
    return jax.shard_map(
        functools.partial(per_device, mesh.shape["bank"], mesh.shape["seg"]),
        mesh=mesh,
        in_specs=placed,
        out_specs=(P("bank", ("grp", "seg")), P(("grp", "seg")), P(("grp", "bank"))),
        check_vma=False,
    )
```
